32 devices in a mesh: dp: 4 (over y, x), expert: 8 (over z, core).
Axes of the slice: x: 2, y: 2, z: 4, core: 2. Of those that a mesh axis runs over, the one named last changes fastest.
Arguments:
- grad_out: bfloat16 [4096, 3072], P(('dp', 'expert')), may hold values from -6 to 6
- expert_ids: int32 [4096, 2], P(('dp', 'expert')), may hold values from 0 to 7, all different within a row; in each aligned block of 128 rows (0 to 127, 128 to 255, ...) at most 36 rows name the same one
- down_weight: bfloat16 [8, 1024, 3072], P('expert'), may hold values from -0.109375 to 0.109375
- history_grad: float32 [8, 8], replicated, may hold values from 0.5 to 3
- history_hidden: float32 [8, 8], replicated, may hold values from 0.5 to 3
Outputs:
- hidden_scaled: bfloat16 [4, 8, 288, 1024], P('dp', 'expert')
- new_history_grad: float32 [8, 8], replicated
- new_history_hidden: float32 [8, 8], replicated
The draws below stay inside these ranges and needn't reach their ends.
Inputs may be any that keep to these rules, and one draw needn't show every extreme that they name: `expert_ids`: each row names 2 different experts; among the 128 rows of one device no expert is named more than 36 times, a bound that some block reaches in some devices.
All inputs are finite; a program needn't handle non-finite values.
Results may differ from the reference program's by a relative error of at most 0.0045.
Values may be sent and summed in bfloat16 or wider, within the bound.
A program may use at most 128 MiB of HBM per device.

```python
import math
import jax
import jax.numpy as jnp
import numpy as np
from jax import lax

D = 3072
EXPERTS = 8
TOP = 2
FF_DEV = 1024
HIST = 8
TOK_DEV = 128
CAP = 36
TOKENS = 4096
N_DP = 4
N_EXPERT = 8


def steps_of(key, dims, split, smallest, top_value):
    level, own = 1.0, jax.random.fold_in(key, 6)
    for axis_at, shards_of in split:
        steps = jnp.exp(jax.random.uniform(jax.random.fold_in(own, axis_at), (shards_of,), jnp.float32, smallest / len(split), top_value / len(split)))
        level = level * jnp.repeat(steps, dims[axis_at] // shards_of).reshape([-1 if axis == axis_at else 1 for axis in range(len(dims))])
    return level


def deal_out(own_key, own, number, rows, number_of, top, bound, lean):
    ranking = jax.random.permutation(own_key, number_of)
    packed, ordinary = portions_of(number_of, rows * top, bound, lean, True), portions_of(number_of, rows * top, bound, lean, False)
    places = jnp.arange(number_of)

    def named(lengths, turn):
        used = int((lengths > 0).sum())
        fixed = max(1, used // 4)
        moved = fixed + (places - fixed + turn * (used - fixed)) % max(1, number_of - fixed)
        return jnp.zeros((number_of,), jnp.int32).at[ranking[jnp.where(places < fixed, places, moved)]].set(jnp.asarray(lengths, jnp.int32))

    lengths = jnp.where(number % 4 == 0, named(packed, number // 4), named(ordinary, number - number // 4 - 1))
    mixed = jax.random.permutation(jax.random.fold_in(own, 3), number_of)
    giver, receiver = mixed[0:number_of // 2 * 2:2], mixed[1:number_of // 2 * 2:2]
    room = jnp.minimum(lengths[giver] - 1, bound - lengths[receiver]) // 2
    room = jnp.where((giver == ranking[0]) | (receiver == ranking[0]) | (lengths[receiver] == 0), 0, jnp.maximum(room, 0))
    moved = jax.random.randint(jax.random.fold_in(own, 4), (number_of // 2,), 0, 1 << 20) % (room + 1)
    lengths = lengths.at[giver].add(-moved).at[receiver].add(moved)
    items = jnp.searchsorted(jnp.cumsum(lengths), jnp.arange(rows * top), side="right").astype(jnp.int32)
    grid = items.reshape(top, rows).T
    grid = grid[jax.random.permutation(jax.random.fold_in(own, 1), rows)]
    turn = jax.random.randint(jax.random.fold_in(own, 2), (rows, 1), 0, top)
    return jnp.take_along_axis(grid, (jnp.arange(top)[None, :] + turn) % top, axis=1)


def portions_of(count, total, bound, slope, full):
    loads = [(1 << 20) // math.isqrt(rank ** slope) + 1 for rank in range(1, count + 1)]
    largest = bound if full else min(bound, max(-(-total // count), total * loads[0] // sum(loads)))
    least = 1 if total - largest >= count - 1 else 0
    given, surplus = [largest] + [least] * (count - 1), total - largest - least * (count - 1)
    while surplus > 0:
        candidates = [i for i in range(1, count) if given[i] < largest] or [i for i in range(1, count) if given[i] < bound]
        mass, budget = sum([loads[i] for i in candidates]), surplus
        for i in candidates:
            extra = min(bound - given[i], max(1, budget * loads[i] // mass), surplus)
            given[i] = given[i] + extra
            surplus = surplus - extra
    return np.array(given)


def centred(own_key, shape, spread, bound, split=(), held_as=jnp.bfloat16):
    result = jax.random.normal(own_key, shape, jnp.float32) * spread
    if len(split) > 0:
        result = steps_of(own_key, shape, split, -0.22, 0.18) * result
    return jnp.clip(result, min=-bound, max=bound).astype(held_as)


def setup_inputs(seed: int = 0) -> dict:
    seeds = jax.random.split(jax.random.key(seed), 6)
    grad_out = centred(seeds[0], (TOKENS, D), 1.0, 6.0, ((0, 32),))
    expert_ids_keys = jax.random.split(jax.random.fold_in(seeds[1], 1), TOKENS // TOK_DEV)
    expert_ids_turns = jax.random.permutation(jax.random.fold_in(seeds[1], 3), TOKENS // TOK_DEV)
    expert_ids = jax.vmap(lambda own, number: deal_out(jax.random.fold_in(seeds[1], 2), own, number, TOK_DEV, EXPERTS, TOP, CAP, 2))(expert_ids_keys, expert_ids_turns).reshape((TOKENS, TOP))
    down_weight = centred(seeds[2], (N_EXPERT, FF_DEV, D), D ** -0.5, 0.109375, ((0, 8),))
    history_grad = jnp.clip(jnp.exp(jax.random.uniform(seeds[3], (HIST, EXPERTS), jnp.float32, math.log(0.5), math.log(3.0))), 0.5, 3.0)
    history_hidden = jnp.clip(jnp.exp(jax.random.uniform(seeds[4], (HIST, EXPERTS), jnp.float32, math.log(0.5), math.log(3.0))), 0.5, 3.0)
    return {"grad_out": grad_out, "expert_ids": expert_ids, "down_weight": down_weight, "history_grad": history_grad, "history_hidden": history_hidden}


def reference(grad_out, expert_ids, down_weight, history_grad, history_hidden):
    slices = N_EXPERT // EXPERTS
    routing = expert_ids.reshape(N_DP, N_EXPERT, TOK_DEV * TOP)
    onehot = (routing[..., None] == jnp.arange(EXPERTS, dtype=jnp.int32)).astype(jnp.int32)
    before = jnp.cumsum(onehot, axis=2) - onehot
    slot_index = jnp.sum(before * onehot, axis=-1).astype(jnp.int32)
    scale_in = 1.0 / jnp.max(history_grad, axis=0)
    scale_hidden = 1.0 / jnp.max(history_hidden, axis=0)
    gradients = grad_out.reshape(N_DP, N_EXPERT, TOK_DEV, D)
    row_peak = jnp.max(jnp.abs(gradients.astype(jnp.float32)), axis=-1)
    routed = jnp.max(onehot.reshape(N_DP, N_EXPERT, TOK_DEV, TOP, EXPERTS), axis=3) > 0
    grad_amax = jnp.max(jnp.where(routed, row_peak[..., None], 0.0), axis=(0, 1, 2))
    token_of = jnp.arange(TOK_DEV * TOP, dtype=jnp.int32) // TOP
    weights = down_weight.reshape(EXPERTS, slices * FF_DEV, D)
    source_index = jnp.broadcast_to(jnp.arange(N_EXPERT, dtype=jnp.int32)[:, None], (N_EXPERT, TOK_DEV * TOP))

    def one_replica(inputs):
        grads_here, routing_here, slots_here = inputs
        token_rows = grads_here[:, token_of].astype(jnp.float32)
        quantized = jnp.clip(token_rows * scale_in[routing_here][..., None], -1.0, 1.0).astype(jnp.bfloat16)
        buffer = jnp.zeros((EXPERTS, N_EXPERT, CAP, D), jnp.bfloat16)
        buffer = buffer.at[routing_here, source_index, slots_here].set(quantized)

        def one_expert(pair):
            expert, block = pair
            received = block.reshape(N_EXPERT * CAP, D)
            product = jnp.dot(received, weights[expert].T, preferred_element_type=jnp.float32)
            hidden = product / scale_in[expert]
            scaled = jnp.clip(hidden * scale_hidden[expert], -1.0, 1.0).astype(jnp.bfloat16)
            scaled = scaled.reshape(N_EXPERT * CAP, slices, FF_DEV).transpose(1, 0, 2)
            return scaled, jnp.max(jnp.abs(hidden))

        scaled, peak_values = lax.map(one_expert, (jnp.arange(EXPERTS, dtype=jnp.int32), buffer))
        return scaled.reshape(N_EXPERT, N_EXPERT * CAP, FF_DEV), peak_values

    hidden_scaled, peak_values = lax.map(one_replica, (gradients, routing, slot_index))
    hidden_amax = jnp.max(peak_values, axis=0)
    new_history_grad = jnp.concatenate([history_grad[1:], grad_amax[None, :]], axis=0)
    new_history_hidden = jnp.concatenate([history_hidden[1:], hidden_amax[None, :]], axis=0)
    return hidden_scaled, new_history_grad, new_history_hidden
```

```python
import functools

import jax
import jax.numpy as jnp
from jax import lax
from jax.experimental import pallas as pl
from jax.experimental.pallas import tpu as pltpu
from jax.sharding import PartitionSpec as P

MESH = pl.DeviceIdType.MESH
PARTS = 4
LANES = 128
RELAY_PARTS = 6


def flip_bits(q, k, count):
    out, bit = 0, 1
    while bit < count:
        a, b = (q // bit) % 2, (k // bit) % 2
        out = out + bit * (a + b - 2 * a * b)
        bit *= 2
    return out


def kernel(
    n_dp, n_exp, experts, capacity,
    grad_hbm, ids_ref, hist_g_ref, hist_h_ref, weight_hbm,
    out_ref, best_ref,
    grad_ref, held, weight, send, send_rest, recv, recv_rest, rest_rows, slots, mine, peaks_in,
    grad_sem, weight_sem, send_sem, recv_sem, send_rest_sem, recv_rest_sem, peak_send_sem, peak_recv_sem,
):
    tokens = grad_ref.shape[0]
    main = send.shape[1]
    slices = n_exp // experts
    chips = n_exp // 2
    my_dp, me = lax.axis_index("dp"), lax.axis_index("expert")
    q0, c0 = me // 2, me % 2
    partner = q0 * 2 + 1 - c0
    own = me // slices
    grad_load = pltpu.make_async_copy(grad_hbm, grad_ref, grad_sem)
    grad_load.start()
    load = pltpu.make_async_copy(weight_hbm.at[0], weight, weight_sem)

    barrier = pltpu.get_barrier_semaphore()

    everyone = n_dp * n_exp
    here = my_dp * n_exp + me

    def greet(j, x):
        peer = (here + j) % everyone
        pl.semaphore_signal(
            barrier, inc=1, device_id=(peer // n_exp, peer % n_exp), device_id_type=MESH
        )
        return x

    lax.fori_loop(1, everyone, greet, 0)

    expert_row = lax.broadcasted_iota(jnp.int32, (LANES, tokens), 0)
    ids = ids_ref[...]
    mask_t = jnp.where((ids[0:1, :] == expert_row) | (ids[1:2, :] == expert_row), 1.0, 0.0)
    row = lax.broadcasted_iota(jnp.int32, (tokens, tokens), 0)
    col = lax.broadcasted_iota(jnp.int32, (tokens, tokens), 1)
    earlier = jnp.where(row < col, 1.0, 0.0).astype(jnp.bfloat16)
    before = jnp.dot(mask_t.astype(jnp.bfloat16), earlier, preferred_element_type=jnp.float32)
    slots[...] = jnp.where(mask_t > 0.5, before, -1.0)
    scale_in = 1.0 / jnp.max(hist_g_ref[...], axis=0, keepdims=True)
    scale_hidden = 1.0 / jnp.max(hist_h_ref[...], axis=0, keepdims=True)
    which = lax.broadcasted_iota(jnp.int32, (1, experts), 1)

    def pick(values, e):
        return jnp.sum(jnp.where(which == e, values, 0.0), axis=1, keepdims=True)

    position = lax.broadcasted_iota(jnp.int32, (capacity, tokens), 0).astype(jnp.float32)

    def prepare(e):
        onehot = jnp.where(slots[pl.ds(e, 1), :] == position, 1.0, 0.0).astype(jnp.bfloat16)
        rows = jnp.dot(onehot, grad_ref[...], preferred_element_type=jnp.float32)
        block = jnp.clip(rows * pick(scale_in, e), -1.0, 1.0)
        send[e] = block[0:main].astype(jnp.bfloat16)
        send_rest[e] = block[main:capacity].astype(jnp.bfloat16)

    span = weight.shape[1] // PARTS

    def outgoing(d, p):
        columns = pl.ds(p * span, span)
        return pltpu.make_async_remote_copy(
            src_ref=send.at[d // slices, :, columns], dst_ref=recv.at[me, :, columns],
            send_sem=send_sem.at[p, d], recv_sem=recv_sem.at[p, me],
            device_id=(my_dp, d), device_id_type=MESH,
        )

    def outgoing_rest(d):
        return pltpu.make_async_remote_copy(
            src_ref=send_rest.at[d // slices], dst_ref=recv_rest.at[me],
            send_sem=send_rest_sem.at[d], recv_sem=recv_rest_sem.at[me],
            device_id=(my_dp, d), device_id_type=MESH,
        )

    def incoming(s, p):
        columns = pl.ds(p * span, span)
        return pltpu.make_async_remote_copy(
            src_ref=send.at[0, :, columns], dst_ref=recv.at[s, :, columns],
            send_sem=send_sem.at[p, s], recv_sem=recv_sem.at[p, s],
            device_id=(my_dp, s), device_id_type=MESH,
        )

    def incoming_rest(s):
        return pltpu.make_async_remote_copy(
            src_ref=send_rest.at[0], dst_ref=recv_rest.at[s],
            send_sem=send_rest_sem.at[s], recv_sem=recv_rest_sem.at[s],
            device_id=(my_dp, s), device_id_type=MESH,
        )

    def chip_of(j):
        k = j
        if chips & (chips - 1) == 0:
            return flip_bits(q0, k, chips)
        return (q0 + k) % chips

    def source_of(j):
        if chips & (chips - 1) == 0:
            return chip_of(j)
        k = j
        return (q0 + chips - k) % chips

    def prepare_pair(q):
        prepare(2 * q + c0)
        prepare(2 * q + 1 - c0)

    def send_pair(q):
        for p in range(PARTS):
            for c in (c0, 1 - c0):
                outgoing(2 * q + c, p).start()
                if p == 0:
                    outgoing_rest(2 * q + c).start()

    greeted = everyone - 1
    grad_load.wait()
    load.start()
    if slices == 1:
        prepare_pair(chip_of(jnp.int32(1)))
        pl.semaphore_wait(barrier, greeted)

        def step(j, x):
            prepare_pair(chip_of((j + 1) % chips))
            send_pair(chip_of(j))
            return x
    else:
        def fill(e, x):
            prepare(e)
            return x

        lax.fori_loop(0, experts, fill, 0)
        pl.semaphore_wait(barrier, greeted)

        def step(j, x):
            send_pair(chip_of(j))
            return x

    lax.fori_loop(1, chips, step, 0)
    for p in range(PARTS):
        outgoing(partner, p).start()
    outgoing_rest(partner).start()

    recv[me] = send[own]
    recv_rest[me] = send_rest[own]
    row_peak = jnp.max(jnp.abs(grad_ref[...]).astype(jnp.float32), axis=1, keepdims=True)
    grad_peak = jnp.max(jnp.where(mask_t.T > 0.5, row_peak, 0.0), axis=0, keepdims=True)

    back = 1.0 / pick(scale_in, own)
    own_hidden = pick(scale_hidden, own)
    load.wait()

    def times_weight(block, columns):
        return lax.dot_general(
            block, weight[:, columns], (((1,), (1,)), ((), ())), preferred_element_type=jnp.float32
        )

    def multiply(block):
        return finish(times_weight(block, slice(None)))

    def finish(product):
        hidden = product * back
        scaled = jnp.clip(hidden * own_hidden, -1.0, 1.0)
        return scaled, jnp.max(jnp.max(jnp.abs(hidden), axis=0, keepdims=True), axis=1, keepdims=True)

    def pair_rows(q):
        return recv[pl.ds(2 * q, 2)].reshape(2 * main, recv.shape[2])

    def put_pair(q, scaled):
        for c in range(2):
            held[2 * q + c] = scaled[c * main:(c + 1) * main].astype(jnp.bfloat16)

    def take_own():
        for p in range(PARTS):
            incoming(partner, p).wait_recv()
        scaled, peak = multiply(pair_rows(q0))
        put_pair(q0, scaled)
        return peak

    def take(j, peak):
        q = source_of(j)
        for p in range(PARTS):
            incoming(2 * q, p).wait_recv()
            incoming(2 * q + 1, p).wait_recv()
        scaled, peak_here = multiply(pair_rows(q))
        put_pair(q, scaled)
        return jnp.maximum(peak, peak_here)

    peak = lax.fori_loop(1, chips - 1, take, take_own())

    def take_rest(j, x):
        incoming_rest((me + j) % n_exp).wait_recv()
        return x

    lax.fori_loop(1, n_exp, take_rest, 0)
    rest = capacity - main
    for s in range(n_exp):
        rest_rows[s * rest:(s + 1) * rest, :] = recv_rest[s].astype(jnp.float32)
    last = source_of(jnp.int32(chips - 1))
    product = None
    for p in range(PARTS):
        incoming(2 * last, p).wait_recv()
        incoming(2 * last + 1, p).wait_recv()
        columns = slice(p * span, (p + 1) * span)
        pair = recv[pl.ds(2 * last, 2), :, columns].reshape(2 * main, span)
        block = jnp.concatenate([pair, rest_rows[:, columns].astype(jnp.bfloat16)], axis=0)
        piece = times_weight(block, columns)
        product = piece if product is None else product + piece
    scaled, peak_here = finish(product)
    peak = jnp.maximum(peak, peak_here)

    at = lax.broadcasted_iota(jnp.int32, (1, LANES), 1)
    hidden_peak = jnp.where(at == own, peak, 0.0)
    part = lax.broadcasted_iota(jnp.int32, (8, LANES), 0)
    mine[...] = jnp.where(part == 0, grad_peak, jnp.where(part == 1, hidden_peak, 0.0))

    def peak_copy(peer, slot, j):
        return pltpu.make_async_remote_copy(
            src_ref=mine, dst_ref=peaks_in.at[slot],
            send_sem=peak_send_sem.at[j], recv_sem=peak_recv_sem.at[slot],
            device_id=(peer // n_exp, peer % n_exp), device_id_type=MESH,
        )

    def peak_start(j, x):
        peak_copy((here + j) % everyone, here, j).start()
        return x

    def peak_fold(j, best):
        peer = (here + j) % everyone
        peak_copy(peer, peer, j).wait_recv()
        return jnp.maximum(best, peaks_in[peer])

    def peak_finish(j, x):
        peak_copy((here + j) % everyone, here, j).wait_send()
        return x

    lax.fori_loop(1, everyone, peak_start, 0)
    put_pair(last, scaled)
    for s in range(n_exp):
        at_row = 2 * main + s * rest
        base = s * capacity
        out_ref[base:base + main, :] = held[s]
        out_ref[base + main:base + capacity, :] = scaled[at_row:at_row + rest].astype(jnp.bfloat16)
    best = lax.fori_loop(1, everyone, peak_fold, mine[...])
    lax.fori_loop(1, everyone, peak_finish, 0)

    best_ref[...] = best

    def drain(j, x):
        for p in range(PARTS):
            outgoing((me + j) % n_exp, p).wait_send()
        outgoing_rest((me + j) % n_exp).wait_send()
        return x

    lax.fori_loop(1, n_exp, drain, 0)


def finish_kernel(hist_g_ref, hist_h_ref, best_ref, out_ref, new_g_ref, new_h_ref, final_ref):
    final_ref[...] = out_ref[...]
    keep = hist_g_ref.shape[0] - 1
    experts = hist_g_ref.shape[1]
    new_g_ref[0:keep, :] = hist_g_ref[1:keep + 1, :]
    new_g_ref[keep:keep + 1, :] = best_ref[0:1, 0:experts]
    new_h_ref[0:keep, :] = hist_h_ref[1:keep + 1, :]
    new_h_ref[keep:keep + 1, :] = best_ref[1:2, 0:experts]


def by_blocks(grad_out, expert_ids, down_weight, history_grad, history_hidden):
    tokens, width = grad_out.shape
    experts = history_grad.shape[1]
    n_dp, n_exp = lax.axis_size("dp"), lax.axis_size("expert")
    capacity = tokens * 9 // 32
    main = (capacity - 1) // 16 * 16
    rest = capacity - main
    units = down_weight.shape[1]
    vmem = pl.BlockSpec(memory_space=pltpu.VMEM)
    dma = pltpu.SemaphoreType.DMA
    out, best = pl.pallas_call(
        functools.partial(kernel, n_dp, n_exp, experts, capacity),
        out_shape=(
            jax.ShapeDtypeStruct((n_exp * capacity, units), jnp.bfloat16),
            jax.ShapeDtypeStruct((8, LANES), jnp.float32),
        ),
        in_specs=[pl.BlockSpec(memory_space=pl.ANY), vmem, vmem, vmem, pl.BlockSpec(memory_space=pl.ANY)],
        out_specs=(vmem, vmem),
        scratch_shapes=[
            pltpu.VMEM((tokens, width), jnp.bfloat16),
            pltpu.VMEM((n_exp, main, units), jnp.bfloat16),
            pltpu.VMEM((units, width), jnp.bfloat16),
            pltpu.VMEM((experts, main, width), jnp.bfloat16),
            pltpu.VMEM((experts, rest, width), jnp.bfloat16),
            pltpu.VMEM((n_exp, main, width), jnp.bfloat16),
            pltpu.VMEM((n_exp, rest, width), jnp.bfloat16),
            pltpu.VMEM((n_exp * rest, width), jnp.float32),
            pltpu.VMEM((LANES, tokens), jnp.float32),
            pltpu.VMEM((8, LANES), jnp.float32),
            pltpu.VMEM((n_dp * n_exp, 8, LANES), jnp.float32),
            dma, dma, dma((PARTS, n_exp)), dma((PARTS, n_exp)), dma((n_exp,)), dma((n_exp,)),
            dma((n_dp * n_exp,)), dma((n_dp * n_exp,)),
        ],
        compiler_params=pltpu.CompilerParams(
            collective_id=0, has_side_effects=True, vmem_limit_bytes=60 * 1024 * 1024
        ),
    )(grad_out, expert_ids.T, history_grad, history_hidden, down_weight)
    new_g, new_h, out = pl.pallas_call(
        finish_kernel,
        out_shape=(
            jax.ShapeDtypeStruct(history_grad.shape, jnp.float32),
            jax.ShapeDtypeStruct(history_hidden.shape, jnp.float32),
            jax.ShapeDtypeStruct(out.shape, out.dtype),
        ),
        in_specs=[vmem, vmem, vmem, vmem],
        out_specs=(vmem, vmem, vmem),
    )(history_grad, history_hidden, best, out)
    return out.reshape(1, 1, n_exp * capacity, units), new_g, new_h


def relay_kernel(
    n_dp, n_exp, experts, capacity, parts,
    grad_hbm, ids_ref, hist_g_ref, hist_h_ref, weight_hbm,
    out_ref, best_ref,
    grad, raw, weight, send, send_rest, far, far_rest, relay, relay_rest, recv, recv_rest,
    rest_rows, acc, slots, slots_in, onehot, mine, peaks_in,
    grad_sem, weight_sem, raw_send, raw_recv, slot_send, slot_recv,
    near_send, near_rest_send, far_send, far_rest_send, near_recv, near_rest_recv,
    relay_send, relay_rest_send, relay_recv, relay_rest_recv, peak_send, peak_recv,
):
    tokens, width = grad.shape
    main = send.shape[1]
    rest = capacity - main
    half = n_exp // 2
    deep = n_exp // 4
    span = width // parts
    last = parts - 1
    my_dp, me = lax.axis_index("dp"), lax.axis_index("expert")
    q0, c0 = me // 2, me % 2
    side = q0 // deep
    base, far_base = side * half, (1 - side) * half
    my_i, my_k = me - base, q0 - side * deep
    inner = q0 == deep - 1 + side
    relay_dev = 2 * (deep - side) + c0
    everyone = n_dp * n_exp
    here = my_dp * n_exp + me

    grad_load = pltpu.make_async_copy(grad_hbm, grad, grad_sem)
    grad_load.start()
    load = pltpu.make_async_copy(weight_hbm.at[0], weight, weight_sem)
    barrier = pltpu.get_barrier_semaphore()

    def greet(j, x):
        peer = (here + j) % everyone
        pl.semaphore_signal(
            barrier, inc=1, device_id=(peer // n_exp, peer % n_exp), device_id_type=MESH
        )
        return x

    lax.fori_loop(1, everyone, greet, 0)

    expert_row = lax.broadcasted_iota(jnp.int32, (LANES, tokens), 0)
    ids = ids_ref[...]
    mask_t = jnp.where((ids[0:1, :] == expert_row) | (ids[1:2, :] == expert_row), 1.0, 0.0)
    row = lax.broadcasted_iota(jnp.int32, (tokens, tokens), 0)
    col = lax.broadcasted_iota(jnp.int32, (tokens, tokens), 1)
    earlier = jnp.where(row < col, 1.0, 0.0).astype(jnp.bfloat16)
    before = jnp.dot(mask_t.astype(jnp.bfloat16), earlier, preferred_element_type=jnp.float32)
    slots[...] = jnp.where(mask_t > 0.5, before, -1.0)
    scale_in = 1.0 / jnp.max(hist_g_ref[...], axis=0, keepdims=True)
    scale_hidden = 1.0 / jnp.max(hist_h_ref[...], axis=0, keepdims=True)
    which = lax.broadcasted_iota(jnp.int32, (1, experts), 1)

    def pick(values, e):
        return jnp.sum(jnp.where(which == e, values, 0.0), axis=1, keepdims=True)

    position = lax.broadcasted_iota(jnp.int32, (main, tokens), 0).astype(jnp.float32)
    rest_row = lax.broadcasted_iota(jnp.int32, (half * rest, tokens), 0)
    rest_position = (rest_row % rest + main).astype(jnp.float32)
    rest_group = rest_row // rest

    def spread(at, slot_row, first):
        spare = jnp.full((half * rest, tokens), -1.0, jnp.float32)
        for i in range(half):
            named = slot_row(first + i)
            onehot[at, i * main:(i + 1) * main, :] = jnp.where(
                named == position, 1.0, 0.0
            ).astype(jnp.bfloat16)
            spare = jnp.where(rest_group == i, named, spare)
        onehot[at, half * main:half * capacity, :] = jnp.where(
            spare == rest_position, 1.0, 0.0
        ).astype(jnp.bfloat16)

    def own_row(e):
        return slots[pl.ds(e, 1), :]

    group_column = lax.broadcasted_iota(jnp.int32, (half * rest, 1), 0) // rest

    def scales_of(first):
        scales = [pick(scale_in, first + i) for i in range(half)]
        spare = jnp.zeros((half * rest, 1), jnp.float32)
        for i in range(half):
            spare = jnp.where(group_column == i, scales[i], spare)
        return scales, spare

    def fill(at, source, scales, put, put_rest):
        rows = jnp.dot(onehot[at], source, preferred_element_type=jnp.float32)
        each, spare = scales
        for i in range(half):
            put(i, jnp.clip(rows[i * main:(i + 1) * main] * each[i], -1.0, 1.0).astype(jnp.bfloat16))
        ends = jnp.clip(rows[half * main:half * capacity] * spare, -1.0, 1.0)
        for i in range(half):
            put_rest(i, ends[i * rest:(i + 1) * rest].astype(jnp.bfloat16))

    def columns_of(p):
        if isinstance(p, int):
            return pl.ds(p * span, span)
        return pl.ds(pl.multiple_of(p * span, span), span)

    def remote(src, dst, send_sem, recv_sem, d):
        return pltpu.make_async_remote_copy(
            src_ref=src, dst_ref=dst, send_sem=send_sem, recv_sem=recv_sem,
            device_id=(my_dp, d), device_id_type=MESH,
        )

    def raw_copy(p, k):
        columns = columns_of(p)
        return remote(
            grad.at[:, columns], raw.at[k, :, columns], raw_send.at[p], raw_recv.at[p, k], relay_dev
        )

    def slot_copy(k):
        return remote(slots.at[pl.ds(0, experts)], slots_in.at[k], slot_send, slot_recv.at[k], relay_dev)

    def near_copy(p, i, at):
        columns = columns_of(p)
        return remote(
            send.at[i, :, columns], recv.at[at, :, columns],
            near_send.at[p, i], near_recv.at[p, at], base + i,
        )

    def near_rest_copy(p, i, at):
        columns = columns_of(p)
        return remote(
            send_rest.at[i, :, columns], recv_rest.at[at, :, columns],
            near_rest_send.at[p, i], near_rest_recv.at[p, at], base + i,
        )

    def far_copy(i, at):
        return remote(
            far.at[i], recv.at[at, :, columns_of(last)],
            far_send.at[i], near_recv.at[last, at], far_base + i,
        )

    def far_rest_copy(i, at):
        return remote(
            far_rest.at[i], recv_rest.at[at, :, columns_of(last)],
            far_rest_send.at[i], near_rest_recv.at[last, at], far_base + i,
        )

    def relay_copy(p, i, c):
        columns = columns_of(p)
        return remote(
            relay.at[i, :, :, columns], recv.at[pl.ds(half + c * deep, deep), :, columns],
            relay_send.at[p, i], relay_recv.at[p, c], base + i,
        )

    def relay_rest_copy(p, i, c):
        columns = columns_of(p)
        return remote(
            relay_rest.at[i, :, :, columns], recv_rest.at[pl.ds(half + c * deep, deep), :, columns],
            relay_rest_send.at[p, i], relay_rest_recv.at[p, c], base + i,
        )

    spread(0, own_row, base)
    spread(1, own_row, far_base)
    near_scales = scales_of(base)
    grad_load.wait()
    load.start()
    pl.semaphore_wait(barrier, everyone - 1)
    slot_copy(my_k).start()
    raw_copy(0, my_k).start()

    @pl.when(inner)
    def _():
        def more(p, x):
            raw_copy(p, my_k).start()
            return x

        lax.fori_loop(1, last, more, 0)

    def direct(p, x):
        columns = columns_of(p)

        def put(i, block):
            send[i, :, columns] = block

        def put_rest(i, block):
            send_rest[i, :, columns] = block

        fill(0, grad[:, columns], near_scales, put, put_rest)
        for j in range(1, half):
            i = (my_i + j) % half
            near_copy(p, i, my_i).start()
            near_rest_copy(p, i, my_i).start()

        @pl.when(jnp.logical_not(inner) & (p + 1 < last))
        def _():
            raw_copy(p + 1, my_k).start()

        return x

    lax.fori_loop(0, parts, direct, 0)

    def put_far(i, block):
        far[i] = block

    def put_far_rest(i, block):
        far_rest[i] = block

    fill(1, grad[:, columns_of(last)], scales_of(far_base), put_far, put_far_rest)
    far_at = half + c0 * deep + my_k
    for i in range(half):
        far_copy(i, far_at).start()
        far_rest_copy(i, far_at).start()

    recv[my_i] = send[my_i]
    recv_rest[my_i] = send_rest[my_i]
    row_peak = jnp.max(jnp.abs(grad[...]).astype(jnp.float32), axis=1, keepdims=True)
    grad_peak = jnp.max(jnp.where(mask_t.T > 0.5, row_peak, 0.0), axis=0, keepdims=True)
    back = 1.0 / pick(scale_in, me)
    own_hidden = pick(scale_hidden, me)
    acc[...] = jnp.zeros_like(acc)

    @pl.when(inner)
    def _():
        for k in range(deep):
            slot_copy(k).wait_recv()
            spread(2 + k, lambda e: slots_in[k, pl.ds(e, 1), :], base)

    load.wait()

    def product_of(p):
        columns = columns_of(p)
        for s in range(n_exp):
            rest_rows[s * rest:(s + 1) * rest, :] = recv_rest[s, :, columns].astype(jnp.float32)
        block = jnp.concatenate(
            [recv[:, :, columns].reshape(n_exp * main, span), rest_rows[...].astype(jnp.bfloat16)], axis=0
        )
        return lax.dot_general(
            block, weight[:, columns], (((1,), (1,)), ((), ())), preferred_element_type=jnp.float32
        )

    def take(p, x):
        columns = columns_of(p)

        @pl.when(inner)
        def _():
            for k in range(deep):
                raw_copy(p, k).wait_recv()

                def put(i, block):
                    relay[i, k, :, columns] = block

                def put_rest(i, block):
                    relay_rest[i, k, :, columns] = block

                fill(2 + k, raw[k, :, columns], near_scales, put, put_rest)
            for j in range(1, half):
                i = (my_i + j) % half
                relay_copy(p, i, c0).start()
                relay_rest_copy(p, i, c0).start()
            for k in range(deep):
                recv[half + c0 * deep + k, :, columns] = relay[my_i, k, :, columns]
                recv_rest[half + c0 * deep + k, :, columns] = relay_rest[my_i, k, :, columns]

        for j in range(1, half):
            i = (my_i + j) % half
            near_copy(p, i, i).wait_recv()
            near_rest_copy(p, i, i).wait_recv()
        relay_copy(p, 0, 1 - c0).wait_recv()
        relay_rest_copy(p, 0, 1 - c0).wait_recv()

        @pl.when(jnp.logical_not(inner))
        def _():
            relay_copy(p, 0, c0).wait_recv()
            relay_rest_copy(p, 0, c0).wait_recv()

        acc[...] = acc[...] + product_of(p)
        return x

    lax.fori_loop(0, last, take, 0)

    for j in range(1, half):
        i = (my_i + j) % half
        near_copy(last, i, i).wait_recv()
        near_rest_copy(last, i, i).wait_recv()
    for at in range(half, n_exp):
        far_copy(0, at).wait_recv()
        far_rest_copy(0, at).wait_recv()
    acc[...] = acc[...] + product_of(last)
    hidden = acc[...] * back
    peak = jnp.max(jnp.max(jnp.abs(hidden), axis=0, keepdims=True), axis=1, keepdims=True)
    lane = lax.broadcasted_iota(jnp.int32, (1, LANES), 1)
    mine[...] = jnp.where(lane < experts, grad_peak, jnp.where(lane == experts + me, peak, 0.0))

    def peak_copy(peer, slot, j):
        return pltpu.make_async_remote_copy(
            src_ref=mine, dst_ref=peaks_in.at[slot],
            send_sem=peak_send.at[j], recv_sem=peak_recv.at[slot],
            device_id=(peer // n_exp, peer % n_exp), device_id_type=MESH,
        )

    def peak_start(j, x):
        peak_copy((here + j) % everyone, here, j).start()
        return x

    lax.fori_loop(1, everyone, peak_start, 0)

    scaled = jnp.clip(acc[...] * back * own_hidden, -1.0, 1.0)
    for at in range(n_exp):
        if at < half:
            block, first = side, at * capacity
        else:
            block, first = 1 - side, ((at - half) % deep * 2 + (at - half) // deep) * capacity
        out_ref[block, first:first + main, :] = scaled[at * main:(at + 1) * main].astype(jnp.bfloat16)
        tail = n_exp * main + at * rest
        out_ref[block, first + main:first + capacity, :] = scaled[tail:tail + rest].astype(jnp.bfloat16)

    def peak_fold(j, best):
        peer = (here + j) % everyone
        peak_copy(peer, peer, j).wait_recv()
        return jnp.maximum(best, peaks_in[peer])

    best_ref[...] = lax.fori_loop(1, everyone, peak_fold, mine[...])

    def peak_finish(j, x):
        peak_copy((here + j) % everyone, here, j).wait_send()
        return x

    lax.fori_loop(1, everyone, peak_finish, 0)
    slot_copy(my_k).wait_send()

    def drain(p, x):
        for j in range(1, half):
            i = (my_i + j) % half
            near_copy(p, i, my_i).wait_send()
            near_rest_copy(p, i, my_i).wait_send()

        @pl.when(p < last)
        def _():
            raw_copy(p, my_k).wait_send()

        @pl.when(inner & (p < last))
        def _():
            for j in range(1, half):
                i = (my_i + j) % half
                relay_copy(p, i, c0).wait_send()
                relay_rest_copy(p, i, c0).wait_send()

        return x

    lax.fori_loop(0, parts, drain, 0)
    for i in range(half):
        far_copy(i, far_at).wait_send()
        far_rest_copy(i, far_at).wait_send()


def relay_finish(hist_g_ref, hist_h_ref, best_ref, out_ref, new_g_ref, new_h_ref, final_ref):
    final_ref[...] = out_ref[...]
    keep = hist_g_ref.shape[0] - 1
    experts = hist_g_ref.shape[1]
    new_g_ref[0:keep, :] = hist_g_ref[1:keep + 1, :]
    new_g_ref[keep:keep + 1, :] = best_ref[0:1, 0:experts]
    new_h_ref[0:keep, :] = hist_h_ref[1:keep + 1, :]
    new_h_ref[keep:keep + 1, :] = best_ref[0:1, experts:2 * experts]


def by_relay(grad_out, expert_ids, down_weight, history_grad, history_hidden):
    tokens, width = grad_out.shape
    experts = history_grad.shape[1]
    n_dp, n_exp = lax.axis_size("dp"), lax.axis_size("expert")
    capacity = tokens * 9 // 32
    main = (capacity - 1) // 16 * 16
    rest = capacity - main
    units = down_weight.shape[1]
    half, deep = n_exp // 2, n_exp // 4
    parts = RELAY_PARTS
    span = width // parts
    everyone = n_dp * n_exp
    vmem = pl.BlockSpec(memory_space=pltpu.VMEM)
    dma = pltpu.SemaphoreType.DMA
    bf16, f32 = jnp.bfloat16, jnp.float32
    out, best = pl.pallas_call(
        functools.partial(relay_kernel, n_dp, n_exp, experts, capacity, parts),
        out_shape=(
            jax.ShapeDtypeStruct((2, half * capacity, units), bf16),
            jax.ShapeDtypeStruct((1, LANES), f32),
        ),
        in_specs=[pl.BlockSpec(memory_space=pl.ANY), vmem, vmem, vmem, pl.BlockSpec(memory_space=pl.ANY)],
        out_specs=(vmem, vmem),
        scratch_shapes=[
            pltpu.VMEM((tokens, width), bf16),
            pltpu.VMEM((deep, tokens, width), bf16),
            pltpu.VMEM((units, width), bf16),
            pltpu.VMEM((half, main, width), bf16),
            pltpu.VMEM((half, rest, width), bf16),
            pltpu.VMEM((half, main, span), bf16),
            pltpu.VMEM((half, rest, span), bf16),
            pltpu.VMEM((half, deep, main, width), bf16),
            pltpu.VMEM((half, deep, rest, width), bf16),
            pltpu.VMEM((n_exp, main, width), bf16),
            pltpu.VMEM((n_exp, rest, width), bf16),
            pltpu.VMEM((n_exp * rest, span), f32),
            pltpu.VMEM((n_exp * capacity, units), f32),
            pltpu.VMEM((LANES, tokens), f32),
            pltpu.VMEM((deep, experts, tokens), f32),
            pltpu.VMEM((2 + deep, half * capacity, tokens), bf16),
            pltpu.VMEM((1, LANES), f32),
            pltpu.VMEM((everyone, 1, LANES), f32),
            dma, dma, dma((parts,)), dma((parts, deep)), dma, dma((deep,)),
            dma((parts, half)), dma((parts, half)), dma((half,)), dma((half,)),
            dma((parts, n_exp)), dma((parts, n_exp)),
            dma((parts, half)), dma((parts, half)), dma((parts, 2)), dma((parts, 2)),
            dma((everyone,)), dma((everyone,)),
        ],
        compiler_params=pltpu.CompilerParams(
            collective_id=1, has_side_effects=True, vmem_limit_bytes=60 * 1024 * 1024
        ),
    )(grad_out, expert_ids.T, history_grad, history_hidden, down_weight)
    new_g, new_h, out = pl.pallas_call(
        relay_finish,
        out_shape=(
            jax.ShapeDtypeStruct(history_grad.shape, f32),
            jax.ShapeDtypeStruct(history_hidden.shape, f32),
            jax.ShapeDtypeStruct(out.shape, out.dtype),
        ),
        in_specs=[vmem, vmem, vmem, vmem],
        out_specs=(vmem, vmem, vmem),
    )(history_grad, history_hidden, best, out)
    return out.reshape(1, 1, n_exp * capacity, units), new_g, new_h


def fits_relay(tokens, width, experts, n_exp):
    capacity = tokens * 9 // 32
    return (
        experts == n_exp and n_exp % 4 == 0 and experts % 8 == 0 and 2 * experts <= LANES
        and tokens % LANES == 0 and width % (RELAY_PARTS * LANES) == 0
        and (n_exp // 2 * capacity) % 16 == 0 and (n_exp // 2 * (capacity % 16)) % 16 == 0
        and 0 < capacity % 16
    )


def per_device(*arguments):
    (tokens, width), experts = arguments[0].shape, arguments[3].shape[1]
    if fits_relay(tokens, width, experts, lax.axis_size("expert")):
        return by_relay(*arguments)
    return by_blocks(*arguments)


def solution(mesh):
    in_specs = (
        P(("dp", "expert"), None),
        P(("dp", "expert"), None),
        P("expert", None, None),
        P(),
        P(),
    )
    out_specs = (P("dp", "expert", None, None), P(), P())
    return jax.shard_map(
        per_device, mesh=mesh, in_specs=in_specs, out_specs=out_specs, check_vma=False
    )
```

```python
import functools

import jax
import jax.numpy as jnp
from jax import lax
from jax.experimental import pallas as pl
from jax.experimental.pallas import tpu as pltpu
from jax.sharding import PartitionSpec as P

MESH = pl.DeviceIdType.MESH
PARTS = 4
LANES = 128
RELAY_CHUNKS = 12
RELAY_DIRECT = 3


def flip_bits(q, k, count):
    out, bit = 0, 1
    while bit < count:
        a, b = (q // bit) % 2, (k // bit) % 2
        out = out + bit * (a + b - 2 * a * b)
        bit *= 2
    return out


def kernel(
    n_dp, n_exp, experts, capacity,
    grad_hbm, ids_ref, hist_g_ref, hist_h_ref, weight_hbm,
    out_ref, best_ref,
    grad_ref, held, weight, send, send_rest, recv, recv_rest, rest_rows, slots, mine, peaks_in,
    grad_sem, weight_sem, send_sem, recv_sem, send_rest_sem, recv_rest_sem, peak_send_sem, peak_recv_sem,
):
    tokens = grad_ref.shape[0]
    main = send.shape[1]
    slices = n_exp // experts
    chips = n_exp // 2
    my_dp, me = lax.axis_index("dp"), lax.axis_index("expert")
    q0, c0 = me // 2, me % 2
    partner = q0 * 2 + 1 - c0
    own = me // slices
    grad_load = pltpu.make_async_copy(grad_hbm, grad_ref, grad_sem)
    grad_load.start()
    load = pltpu.make_async_copy(weight_hbm.at[0], weight, weight_sem)

    barrier = pltpu.get_barrier_semaphore()

    everyone = n_dp * n_exp
    here = my_dp * n_exp + me

    def greet(j, x):
        peer = (here + j) % everyone
        pl.semaphore_signal(
            barrier, inc=1, device_id=(peer // n_exp, peer % n_exp), device_id_type=MESH
        )
        return x

    lax.fori_loop(1, everyone, greet, 0)

    expert_row = lax.broadcasted_iota(jnp.int32, (LANES, tokens), 0)
    ids = ids_ref[...]
    mask_t = jnp.where((ids[0:1, :] == expert_row) | (ids[1:2, :] == expert_row), 1.0, 0.0)
    row = lax.broadcasted_iota(jnp.int32, (tokens, tokens), 0)
    col = lax.broadcasted_iota(jnp.int32, (tokens, tokens), 1)
    earlier = jnp.where(row < col, 1.0, 0.0).astype(jnp.bfloat16)
    before = jnp.dot(mask_t.astype(jnp.bfloat16), earlier, preferred_element_type=jnp.float32)
    slots[...] = jnp.where(mask_t > 0.5, before, -1.0)
    scale_in = 1.0 / jnp.max(hist_g_ref[...], axis=0, keepdims=True)
    scale_hidden = 1.0 / jnp.max(hist_h_ref[...], axis=0, keepdims=True)
    which = lax.broadcasted_iota(jnp.int32, (1, experts), 1)

    def pick(values, e):
        return jnp.sum(jnp.where(which == e, values, 0.0), axis=1, keepdims=True)

    position = lax.broadcasted_iota(jnp.int32, (capacity, tokens), 0).astype(jnp.float32)

    def prepare(e):
        onehot = jnp.where(slots[pl.ds(e, 1), :] == position, 1.0, 0.0).astype(jnp.bfloat16)
        rows = jnp.dot(onehot, grad_ref[...], preferred_element_type=jnp.float32)
        block = jnp.clip(rows * pick(scale_in, e), -1.0, 1.0)
        send[e] = block[0:main].astype(jnp.bfloat16)
        send_rest[e] = block[main:capacity].astype(jnp.bfloat16)

    span = weight.shape[1] // PARTS

    def outgoing(d, p):
        columns = pl.ds(p * span, span)
        return pltpu.make_async_remote_copy(
            src_ref=send.at[d // slices, :, columns], dst_ref=recv.at[me, :, columns],
            send_sem=send_sem.at[p, d], recv_sem=recv_sem.at[p, me],
            device_id=(my_dp, d), device_id_type=MESH,
        )

    def outgoing_rest(d):
        return pltpu.make_async_remote_copy(
            src_ref=send_rest.at[d // slices], dst_ref=recv_rest.at[me],
            send_sem=send_rest_sem.at[d], recv_sem=recv_rest_sem.at[me],
            device_id=(my_dp, d), device_id_type=MESH,
        )

    def incoming(s, p):
        columns = pl.ds(p * span, span)
        return pltpu.make_async_remote_copy(
            src_ref=send.at[0, :, columns], dst_ref=recv.at[s, :, columns],
            send_sem=send_sem.at[p, s], recv_sem=recv_sem.at[p, s],
            device_id=(my_dp, s), device_id_type=MESH,
        )

    def incoming_rest(s):
        return pltpu.make_async_remote_copy(
            src_ref=send_rest.at[0], dst_ref=recv_rest.at[s],
            send_sem=send_rest_sem.at[s], recv_sem=recv_rest_sem.at[s],
            device_id=(my_dp, s), device_id_type=MESH,
        )

    def chip_of(j):
        k = j
        if chips & (chips - 1) == 0:
            return flip_bits(q0, k, chips)
        return (q0 + k) % chips

    def source_of(j):
        if chips & (chips - 1) == 0:
            return chip_of(j)
        k = j
        return (q0 + chips - k) % chips

    def prepare_pair(q):
        prepare(2 * q + c0)
        prepare(2 * q + 1 - c0)

    def send_pair(q):
        for p in range(PARTS):
            for c in (c0, 1 - c0):
                outgoing(2 * q + c, p).start()
                if p == 0:
                    outgoing_rest(2 * q + c).start()

    greeted = everyone - 1
    grad_load.wait()
    load.start()
    if slices == 1:
        prepare_pair(chip_of(jnp.int32(1)))
        pl.semaphore_wait(barrier, greeted)

        def step(j, x):
            prepare_pair(chip_of((j + 1) % chips))
            send_pair(chip_of(j))
            return x
    else:
        def fill(e, x):
            prepare(e)
            return x

        lax.fori_loop(0, experts, fill, 0)
        pl.semaphore_wait(barrier, greeted)

        def step(j, x):
            send_pair(chip_of(j))
            return x

    lax.fori_loop(1, chips, step, 0)
    for p in range(PARTS):
        outgoing(partner, p).start()
    outgoing_rest(partner).start()

    recv[me] = send[own]
    recv_rest[me] = send_rest[own]
    row_peak = jnp.max(jnp.abs(grad_ref[...]).astype(jnp.float32), axis=1, keepdims=True)
    grad_peak = jnp.max(jnp.where(mask_t.T > 0.5, row_peak, 0.0), axis=0, keepdims=True)

    back = 1.0 / pick(scale_in, own)
    own_hidden = pick(scale_hidden, own)
    load.wait()

    def times_weight(block, columns):
        return lax.dot_general(
            block, weight[:, columns], (((1,), (1,)), ((), ())), preferred_element_type=jnp.float32
        )

    def multiply(block):
        return finish(times_weight(block, slice(None)))

    def finish(product):
        hidden = product * back
        scaled = jnp.clip(hidden * own_hidden, -1.0, 1.0)
        return scaled, jnp.max(jnp.max(jnp.abs(hidden), axis=0, keepdims=True), axis=1, keepdims=True)

    def pair_rows(q):
        return recv[pl.ds(2 * q, 2)].reshape(2 * main, recv.shape[2])

    def put_pair(q, scaled):
        for c in range(2):
            held[2 * q + c] = scaled[c * main:(c + 1) * main].astype(jnp.bfloat16)

    def take_own():
        for p in range(PARTS):
            incoming(partner, p).wait_recv()
        scaled, peak = multiply(pair_rows(q0))
        put_pair(q0, scaled)
        return peak

    def take(j, peak):
        q = source_of(j)
        for p in range(PARTS):
            incoming(2 * q, p).wait_recv()
            incoming(2 * q + 1, p).wait_recv()
        scaled, peak_here = multiply(pair_rows(q))
        put_pair(q, scaled)
        return jnp.maximum(peak, peak_here)

    peak = lax.fori_loop(1, chips - 1, take, take_own())

    def take_rest(j, x):
        incoming_rest((me + j) % n_exp).wait_recv()
        return x

    lax.fori_loop(1, n_exp, take_rest, 0)
    rest = capacity - main
    for s in range(n_exp):
        rest_rows[s * rest:(s + 1) * rest, :] = recv_rest[s].astype(jnp.float32)
    last = source_of(jnp.int32(chips - 1))
    product = None
    for p in range(PARTS):
        incoming(2 * last, p).wait_recv()
        incoming(2 * last + 1, p).wait_recv()
        columns = slice(p * span, (p + 1) * span)
        pair = recv[pl.ds(2 * last, 2), :, columns].reshape(2 * main, span)
        block = jnp.concatenate([pair, rest_rows[:, columns].astype(jnp.bfloat16)], axis=0)
        piece = times_weight(block, columns)
        product = piece if product is None else product + piece
    scaled, peak_here = finish(product)
    peak = jnp.maximum(peak, peak_here)

    at = lax.broadcasted_iota(jnp.int32, (1, LANES), 1)
    hidden_peak = jnp.where(at == own, peak, 0.0)
    part = lax.broadcasted_iota(jnp.int32, (8, LANES), 0)
    mine[...] = jnp.where(part == 0, grad_peak, jnp.where(part == 1, hidden_peak, 0.0))

    def peak_copy(peer, slot, j):
        return pltpu.make_async_remote_copy(
            src_ref=mine, dst_ref=peaks_in.at[slot],
            send_sem=peak_send_sem.at[j], recv_sem=peak_recv_sem.at[slot],
            device_id=(peer // n_exp, peer % n_exp), device_id_type=MESH,
        )

    def peak_start(j, x):
        peak_copy((here + j) % everyone, here, j).start()
        return x

    def peak_fold(j, best):
        peer = (here + j) % everyone
        peak_copy(peer, peer, j).wait_recv()
        return jnp.maximum(best, peaks_in[peer])

    def peak_finish(j, x):
        peak_copy((here + j) % everyone, here, j).wait_send()
        return x

    lax.fori_loop(1, everyone, peak_start, 0)
    put_pair(last, scaled)
    for s in range(n_exp):
        at_row = 2 * main + s * rest
        base = s * capacity
        out_ref[base:base + main, :] = held[s]
        out_ref[base + main:base + capacity, :] = scaled[at_row:at_row + rest].astype(jnp.bfloat16)
    best = lax.fori_loop(1, everyone, peak_fold, mine[...])
    lax.fori_loop(1, everyone, peak_finish, 0)

    best_ref[...] = best

    def drain(j, x):
        for p in range(PARTS):
            outgoing((me + j) % n_exp, p).wait_send()
        outgoing_rest((me + j) % n_exp).wait_send()
        return x

    lax.fori_loop(1, n_exp, drain, 0)


def finish_kernel(hist_g_ref, hist_h_ref, best_ref, out_ref, new_g_ref, new_h_ref, final_ref):
    final_ref[...] = out_ref[...]
    keep = hist_g_ref.shape[0] - 1
    experts = hist_g_ref.shape[1]
    new_g_ref[0:keep, :] = hist_g_ref[1:keep + 1, :]
    new_g_ref[keep:keep + 1, :] = best_ref[0:1, 0:experts]
    new_h_ref[0:keep, :] = hist_h_ref[1:keep + 1, :]
    new_h_ref[keep:keep + 1, :] = best_ref[1:2, 0:experts]


def by_blocks(grad_out, expert_ids, down_weight, history_grad, history_hidden):
    tokens, width = grad_out.shape
    experts = history_grad.shape[1]
    n_dp, n_exp = lax.axis_size("dp"), lax.axis_size("expert")
    capacity = tokens * 9 // 32
    main = (capacity - 1) // 16 * 16
    rest = capacity - main
    units = down_weight.shape[1]
    vmem = pl.BlockSpec(memory_space=pltpu.VMEM)
    dma = pltpu.SemaphoreType.DMA
    out, best = pl.pallas_call(
        functools.partial(kernel, n_dp, n_exp, experts, capacity),
        out_shape=(
            jax.ShapeDtypeStruct((n_exp * capacity, units), jnp.bfloat16),
            jax.ShapeDtypeStruct((8, LANES), jnp.float32),
        ),
        in_specs=[pl.BlockSpec(memory_space=pl.ANY), vmem, vmem, vmem, pl.BlockSpec(memory_space=pl.ANY)],
        out_specs=(vmem, vmem),
        scratch_shapes=[
            pltpu.VMEM((tokens, width), jnp.bfloat16),
            pltpu.VMEM((n_exp, main, units), jnp.bfloat16),
            pltpu.VMEM((units, width), jnp.bfloat16),
            pltpu.VMEM((experts, main, width), jnp.bfloat16),
            pltpu.VMEM((experts, rest, width), jnp.bfloat16),
            pltpu.VMEM((n_exp, main, width), jnp.bfloat16),
            pltpu.VMEM((n_exp, rest, width), jnp.bfloat16),
            pltpu.VMEM((n_exp * rest, width), jnp.float32),
            pltpu.VMEM((LANES, tokens), jnp.float32),
            pltpu.VMEM((8, LANES), jnp.float32),
            pltpu.VMEM((n_dp * n_exp, 8, LANES), jnp.float32),
            dma, dma, dma((PARTS, n_exp)), dma((PARTS, n_exp)), dma((n_exp,)), dma((n_exp,)),
            dma((n_dp * n_exp,)), dma((n_dp * n_exp,)),
        ],
        compiler_params=pltpu.CompilerParams(
            collective_id=0, has_side_effects=True, vmem_limit_bytes=60 * 1024 * 1024
        ),
    )(grad_out, expert_ids.T, history_grad, history_hidden, down_weight)
    new_g, new_h, out = pl.pallas_call(
        finish_kernel,
        out_shape=(
            jax.ShapeDtypeStruct(history_grad.shape, jnp.float32),
            jax.ShapeDtypeStruct(history_hidden.shape, jnp.float32),
            jax.ShapeDtypeStruct(out.shape, out.dtype),
        ),
        in_specs=[vmem, vmem, vmem, vmem],
        out_specs=(vmem, vmem, vmem),
    )(history_grad, history_hidden, best, out)
    return out.reshape(1, 1, n_exp * capacity, units), new_g, new_h


def relay_kernel(
    n_dp, n_exp, experts, capacity, chunks,
    grad_hbm, ids_hbm, hist_g_hbm, hist_h_hbm, weight_hbm,
    out_ref, best_ref,
    grad, ids_ref, hist_g_ref, hist_h_ref, raw, weight,
    send, send_rest, far, far_rest, relay, relay_rest, recv, recv_rest,
    rest_rows, acc, slots, slots_in, onehot, mine, peaks_in,
    load_sem, known, slot_send, slot_recv, raw_send, raw_recv,
    near_send, near_rest_send, far_send, far_rest_send, relay_send, relay_rest_send,
    main_recv, rest_recv, peak_send, peak_recv,
):
    tokens, width = grad.shape
    main = send.shape[1]
    rest = capacity - main
    half, deep = n_exp // 2, n_exp // 4
    relayed = raw.shape[2]
    span = width // chunks
    hops = relayed // span
    my_dp, me = lax.axis_index("dp"), lax.axis_index("expert")
    q0, c0 = me // 2, me % 2
    side = q0 // deep
    base, far_base = side * half, (1 - side) * half
    my_i, my_k = me - base, q0 - side * deep
    inner = q0 == deep - 1 + side
    outer = jnp.logical_not(inner)
    partner = q0 * 2 + 1 - c0
    across = 2 * (deep - side) + c0
    behind = 2 * (deep - 1 + side + jnp.where(inner, 2 * side - 1, 0)) + c0
    everyone = n_dp * n_exp
    here = my_dp * n_exp + me

    def loading(src, dst, at):
        return pltpu.make_async_copy(src, dst, load_sem.at[at])

    small = (
        loading(ids_hbm, ids_ref, 0), loading(hist_g_hbm, hist_g_ref, 1), loading(hist_h_hbm, hist_h_ref, 2)
    )
    grad_load = loading(grad_hbm, grad, 3)
    load = loading(weight_hbm.at[0], weight, 4)
    for copy in small:
        copy.start()
    grad_load.start()

    def tell(semaphore, d, dp=None):
        pl.semaphore_signal(
            semaphore, inc=1, device_id=(my_dp if dp is None else dp, d), device_id_type=MESH
        )

    barrier = pltpu.get_barrier_semaphore()

    @pl.when(inner)
    def _():
        tell(barrier, across)
        tell(barrier, behind)

    tell(barrier, partner)
    for d in range(1, n_dp):
        tell(barrier, me, (my_dp + d) % n_dp)

    expert_row = lax.broadcasted_iota(jnp.int32, (LANES, tokens), 0)
    row = lax.broadcasted_iota(jnp.int32, (tokens, tokens), 0)
    col = lax.broadcasted_iota(jnp.int32, (tokens, tokens), 1)
    earlier = jnp.where(row < col, 1.0, 0.0).astype(jnp.bfloat16)
    for copy in small:
        copy.wait()
    ids = ids_ref[...]
    mask_t = jnp.where((ids[0:1, :] == expert_row) | (ids[1:2, :] == expert_row), 1.0, 0.0)
    before = jnp.dot(mask_t.astype(jnp.bfloat16), earlier, preferred_element_type=jnp.float32)
    slots[...] = jnp.where(mask_t > 0.5, before, -1.0)
    scale_in = 1.0 / jnp.max(hist_g_ref[...], axis=0, keepdims=True)
    scale_hidden = 1.0 / jnp.max(hist_h_ref[...], axis=0, keepdims=True)
    which = lax.broadcasted_iota(jnp.int32, (1, experts), 1)

    def pick(values, e):
        return jnp.sum(jnp.where(which == e, values, 0.0), axis=1, keepdims=True)

    position = lax.broadcasted_iota(jnp.int32, (main, tokens), 0).astype(jnp.float32)
    rest_row = lax.broadcasted_iota(jnp.int32, (half * rest, tokens), 0)
    rest_position = (rest_row % rest + main).astype(jnp.float32)
    rest_group = rest_row // rest

    def spread(at, slot_row, first):
        spare = jnp.full((half * rest, tokens), -1.0, jnp.float32)
        for i in range(half):
            named = slot_row(first + i)
            onehot[at, i * main:(i + 1) * main, :] = jnp.where(
                named == position, 1.0, 0.0
            ).astype(jnp.bfloat16)
            spare = jnp.where(rest_group == i, named, spare)
        onehot[at, half * main:half * capacity, :] = jnp.where(
            spare == rest_position, 1.0, 0.0
        ).astype(jnp.bfloat16)

    def own_row(e):
        return slots[pl.ds(e, 1), :]

    group_column = lax.broadcasted_iota(jnp.int32, (half * rest, 1), 0) // rest

    def scales_of(first):
        scales = [pick(scale_in, first + i) for i in range(half)]
        spare = jnp.zeros((half * rest, 1), jnp.float32)
        for i in range(half):
            spare = jnp.where(group_column == i, scales[i], spare)
        return scales, spare

    def fill(at, source, scales, put, put_rest):
        rows = jnp.dot(onehot[at], source, preferred_element_type=jnp.float32)
        each, spare = scales
        for i in range(half):
            put(i, jnp.clip(rows[i * main:(i + 1) * main] * each[i], -1.0, 1.0).astype(jnp.bfloat16))
        ends = jnp.clip(rows[half * main:half * capacity] * spare, -1.0, 1.0)
        for i in range(half):
            put_rest(i, ends[i * rest:(i + 1) * rest].astype(jnp.bfloat16))

    def columns_of(p):
        return pl.ds(pl.multiple_of(p * span, span), span)

    def remote(src, dst, send_sem, recv_sem, d):
        return pltpu.make_async_remote_copy(
            src_ref=src, dst_ref=dst, send_sem=send_sem, recv_sem=recv_sem,
            device_id=(my_dp, d), device_id_type=MESH,
        )

    def sent(ref, send_sem):
        remote(ref, ref, send_sem, send_sem, partner).wait_send()

    def came(ref, recv_sem):
        remote(ref, ref, recv_sem, recv_sem, partner).wait_recv()

    def send_raw(p):
        columns = columns_of(p)
        remote(
            grad.at[:, columns], raw.at[my_k, :, columns], raw_send, raw_recv.at[p], across
        ).start()

    def send_slots():
        remote(slots.at[pl.ds(0, experts)], slots_in.at[my_k], slot_send, slot_recv, across).start()

    def send_near(p):
        columns = columns_of(p)
        for j in range(1, half):
            i = (my_i + j) % half
            remote(
                send.at[i, :, columns], recv.at[my_i, :, columns], near_send, main_recv.at[p], base + i
            ).start()
            remote(
                send_rest.at[i, :, columns], recv_rest.at[my_i, :, columns],
                near_rest_send, rest_recv.at[p], base + i,
            ).start()

    def send_far(p):
        columns, at = columns_of(p), half + c0 * deep + my_k
        for j in range(half):
            i = (my_i + j) % half
            remote(
                far.at[i, :, columns_of(p - hops)], recv.at[at, :, columns],
                far_send, main_recv.at[p], far_base + i,
            ).start()
            remote(
                far_rest.at[i, :, columns_of(p - hops)], recv_rest.at[at, :, columns],
                far_rest_send, rest_recv.at[p], far_base + i,
            ).start()

    def send_relay(p):
        columns, at = columns_of(p), pl.ds(half + c0 * deep, deep)
        for j in range(1, half):
            i = (my_i + j) % half
            remote(
                relay.at[i, :, :, columns], recv.at[at, :, columns],
                relay_send, main_recv.at[p], base + i,
            ).start()
            remote(
                relay_rest.at[i, :, :, columns], recv_rest.at[at, :, columns],
                relay_rest_send, rest_recv.at[p], base + i,
            ).start()

    def wait_chunk(p, senders):
        columns = columns_of(p)
        came(recv.at[pl.ds(0, senders), :, columns], main_recv.at[p])
        came(recv_rest.at[pl.ds(0, senders), :, columns], rest_recv.at[p])

    spread(0, own_row, base)
    spread(1, own_row, far_base)
    near_scales = scales_of(base)
    grad_load.wait()
    load.start()
    pl.semaphore_wait(barrier, n_dp + 1)
    tell(known.at[0], partner)

    @pl.when(inner)
    def _():
        tell(known.at[0], across)
        send_slots()

        def more(p, x):
            send_raw(p)
            return x

        lax.fori_loop(0, hops, more, 0)
        pl.semaphore_wait(known.at[0], 3)
        tell(known.at[1], across)
        tell(known.at[1], behind)

    @pl.when(outer)
    def _():
        tell(known.at[0], behind)
        pl.semaphore_wait(known.at[0], 1)

    def direct(p, x):
        columns = columns_of(p)

        def put(i, block):
            send[i, :, columns] = block

        def put_rest(i, block):
            send_rest[i, :, columns] = block

        fill(0, grad[:, columns], near_scales, put, put_rest)
        send_near(p)

        @pl.when(p == 0)
        def _():
            pl.semaphore_wait(known.at[1], 1)

            @pl.when(inner)
            def _():
                tell(known.at[2], behind)

            @pl.when(outer)
            def _():
                send_slots()

        @pl.when(outer & (p < hops))
        def _():
            send_raw(p)

        return x

    lax.fori_loop(0, chunks, direct, 0)

    @pl.when(outer)
    def _():
        pl.semaphore_wait(known.at[2], 1)

    far_scales = scales_of(far_base)

    def directly_far(p, x):
        columns = columns_of(p - hops)

        def put(i, block):
            far[i, :, columns] = block

        def put_rest(i, block):
            far_rest[i, :, columns] = block

        fill(1, grad[:, columns_of(p)], far_scales, put, put_rest)
        send_far(p)
        return x

    lax.fori_loop(hops, chunks, directly_far, 0)
    recv[my_i] = send[my_i]
    recv_rest[my_i] = send_rest[my_i]
    row_peak = jnp.max(jnp.abs(grad[...]).astype(jnp.float32), axis=1, keepdims=True)
    grad_peak = jnp.max(jnp.where(mask_t.T > 0.5, row_peak, 0.0), axis=0, keepdims=True)
    back = 1.0 / pick(scale_in, me)
    own_hidden = pick(scale_hidden, me)
    acc[...] = jnp.zeros_like(acc)

    @pl.when(inner)
    def _():
        came(slots_in, slot_recv)
        for k in range(deep):
            spread(2 + k, lambda e: slots_in[k, pl.ds(e, 1), :], base)

    load.wait()

    def product_of(p):
        columns = columns_of(p)
        for s in range(n_exp):
            rest_rows[s * rest:(s + 1) * rest, :] = recv_rest[s, :, columns].astype(jnp.float32)
        block = jnp.concatenate(
            [recv[:, :, columns].reshape(n_exp * main, span), rest_rows[...].astype(jnp.bfloat16)], axis=0
        )
        return lax.dot_general(
            block, weight[:, columns], (((1,), (1,)), ((), ())), preferred_element_type=jnp.float32
        )

    def take(p, x):
        columns = columns_of(p)

        @pl.when(inner)
        def _():
            came(raw.at[:, :, columns], raw_recv.at[p])
            for k in range(deep):

                def put(i, block):
                    relay[i, k, :, columns] = block

                def put_rest(i, block):
                    relay_rest[i, k, :, columns] = block

                fill(2 + k, raw[k, :, columns], near_scales, put, put_rest)
            send_relay(p)
            for k in range(deep):
                recv[half + c0 * deep + k, :, columns] = relay[my_i, k, :, columns]
                recv_rest[half + c0 * deep + k, :, columns] = relay_rest[my_i, k, :, columns]
            wait_chunk(p, half - 1 + deep)

        @pl.when(outer)
        def _():
            wait_chunk(p, n_exp - 1)

        acc[...] = acc[...] + product_of(p)
        return x

    lax.fori_loop(0, hops, take, 0)

    def take_tail(p, x):
        wait_chunk(p, n_exp - 1)
        acc[...] = acc[...] + product_of(p)
        return x

    lax.fori_loop(hops, chunks, take_tail, 0)
    hidden = acc[...] * back
    peak = jnp.max(jnp.max(jnp.abs(hidden), axis=0, keepdims=True), axis=1, keepdims=True)
    lane = lax.broadcasted_iota(jnp.int32, (1, LANES), 1)
    mine[...] = jnp.where(lane < experts, grad_peak, jnp.where(lane == experts + me, peak, 0.0))
    for k in range(n_exp // 2 - 1, -1, -1):
        for c in (c0, 1 - c0):
            for d in range(n_dp):
                if k == 0 and c is c0 and d == 0:
                    continue
                pltpu.make_async_remote_copy(
                    src_ref=mine, dst_ref=peaks_in.at[here], send_sem=peak_send, recv_sem=peak_recv,
                    device_id=((my_dp + d) % n_dp, 2 * flip_bits(q0, k, n_exp // 2) + c), device_id_type=MESH,
                ).start()
    peaks_in[here] = mine[...]
    scaled = jnp.clip(acc[...] * back * own_hidden, -1.0, 1.0)
    for at in range(n_exp):
        if at < half:
            block, first = side, at * capacity
        else:
            block, first = 1 - side, ((at - half) % deep * 2 + (at - half) // deep) * capacity
        out_ref[block, first:first + main, :] = scaled[at * main:(at + 1) * main].astype(jnp.bfloat16)
        tail = n_exp * main + at * rest
        out_ref[block, first + main:first + capacity, :] = scaled[tail:tail + rest].astype(jnp.bfloat16)

    sent(slots.at[pl.ds(0, experts)], slot_send)
    sent(grad.at[:, pl.ds(0, relayed)], raw_send)
    sent(send.at[pl.ds(0, half - 1)], near_send)
    sent(send_rest.at[pl.ds(0, half - 1)], near_rest_send)
    sent(far, far_send)
    sent(far_rest, far_rest_send)

    @pl.when(inner)
    def _():
        sent(relay.at[pl.ds(0, half - 1)], relay_send)
        sent(relay_rest.at[pl.ds(0, half - 1)], relay_rest_send)

    others = peaks_in.at[pl.ds(0, everyone - 1)]
    sent(others, peak_send)
    came(others, peak_recv)
    best_ref[...] = jnp.max(peaks_in[...], axis=0)


def relay_finish(hist_g_ref, hist_h_ref, best_ref, out_ref, new_g_ref, new_h_ref, final_hbm, sem):
    copy = pltpu.make_async_copy(out_ref, final_hbm, sem)
    copy.start()
    keep = hist_g_ref.shape[0] - 1
    experts = hist_g_ref.shape[1]
    new_g_ref[0:keep, :] = hist_g_ref[1:keep + 1, :]
    new_g_ref[keep:keep + 1, :] = best_ref[0:1, 0:experts]
    new_h_ref[0:keep, :] = hist_h_ref[1:keep + 1, :]
    new_h_ref[keep:keep + 1, :] = best_ref[0:1, experts:2 * experts]
    copy.wait()


def by_relay(grad_out, expert_ids, down_weight, history_grad, history_hidden):
    tokens, width = grad_out.shape
    experts = history_grad.shape[1]
    n_dp, n_exp = lax.axis_size("dp"), lax.axis_size("expert")
    capacity = tokens * 9 // 32
    main = (capacity - 1) // 16 * 16
    rest = capacity - main
    units = down_weight.shape[1]
    half, deep = n_exp // 2, n_exp // 4
    chunks = RELAY_CHUNKS
    span = width // chunks
    tail = RELAY_DIRECT * span
    relayed = width - tail
    everyone = n_dp * n_exp
    vmem, anywhere = pl.BlockSpec(memory_space=pltpu.VMEM), pl.BlockSpec(memory_space=pl.ANY)
    dma = pltpu.SemaphoreType.DMA
    bf16, f32 = jnp.bfloat16, jnp.float32
    out, best = pl.pallas_call(
        functools.partial(relay_kernel, n_dp, n_exp, experts, capacity, chunks),
        out_shape=(pltpu.VMEM((2, half * capacity, units), bf16), pltpu.VMEM((1, LANES), f32)),
        in_specs=[anywhere] * 5,
        out_specs=(vmem, vmem),
        scratch_shapes=[
            pltpu.VMEM((tokens, width), bf16),
            pltpu.VMEM(expert_ids.shape[::-1], jnp.int32),
            pltpu.VMEM(history_grad.shape, f32),
            pltpu.VMEM(history_hidden.shape, f32),
            pltpu.VMEM((deep, tokens, relayed), bf16),
            pltpu.VMEM((units, width), bf16),
            pltpu.VMEM((half, main, width), bf16),
            pltpu.VMEM((half, rest, width), bf16),
            pltpu.VMEM((half, main, tail), bf16),
            pltpu.VMEM((half, rest, tail), bf16),
            pltpu.VMEM((half, deep, main, relayed), bf16),
            pltpu.VMEM((half, deep, rest, relayed), bf16),
            pltpu.VMEM((n_exp, main, width), bf16),
            pltpu.VMEM((n_exp, rest, width), bf16),
            pltpu.VMEM((n_exp * rest, span), f32),
            pltpu.VMEM((n_exp * capacity, units), f32),
            pltpu.VMEM((LANES, tokens), f32),
            pltpu.VMEM((deep, experts, tokens), f32),
            pltpu.VMEM((2 + deep, half * capacity, tokens), bf16),
            pltpu.VMEM((1, LANES), f32),
            pltpu.VMEM((everyone, 1, LANES), f32),
            dma((5,)), pltpu.SemaphoreType.REGULAR((3,)), dma, dma, dma, dma((relayed // span,)),
            dma, dma, dma, dma, dma, dma,
            dma((chunks,)), dma((chunks,)), dma, dma,
        ],
        compiler_params=pltpu.CompilerParams(
            collective_id=1, has_side_effects=True, vmem_limit_bytes=56 * 1024 * 1024
        ),
    )(grad_out, expert_ids.T, history_grad, history_hidden, down_weight)
    new_g, new_h, out = pl.pallas_call(
        relay_finish,
        out_shape=(
            jax.ShapeDtypeStruct(history_grad.shape, f32),
            jax.ShapeDtypeStruct(history_hidden.shape, f32),
            jax.ShapeDtypeStruct((2, half * capacity, units), bf16),
        ),
        in_specs=[vmem, vmem, vmem, vmem],
        out_specs=(vmem, vmem, anywhere),
        scratch_shapes=[dma],
        compiler_params=pltpu.CompilerParams(vmem_limit_bytes=4 * 1024 * 1024),
    )(history_grad, history_hidden, best, out)
    return out.reshape(1, 1, n_exp * capacity, units), new_g, new_h


def fits_relay(tokens, width, experts, n_exp):
    capacity = tokens * 9 // 32
    return (
        experts == n_exp and n_exp // 4 == 2 and experts % 8 == 0 and 2 * experts <= LANES
        and tokens % LANES == 0 and width % (RELAY_CHUNKS * LANES) == 0
        and (n_exp // 2 * capacity) % 16 == 0 and (n_exp // 2 * (capacity % 16)) % 16 == 0
        and 0 < capacity % 16
    )


def per_device(*arguments):
    (tokens, width), experts = arguments[0].shape, arguments[3].shape[1]
    if fits_relay(tokens, width, experts, lax.axis_size("expert")):
        return by_relay(*arguments)
    return by_blocks(*arguments)


def solution(mesh):
    in_specs = (
        P(("dp", "expert"), None),
        P(("dp", "expert"), None),
        P("expert", None, None),
        P(),
        P(),
    )
    out_specs = (P("dp", "expert", None, None), P(), P())
    return jax.shard_map(
        per_device, mesh=mesh, in_specs=in_specs, out_specs=out_specs, check_vma=False
    )
```

```python
import functools

import jax
import jax.numpy as jnp
from jax import lax
from jax.experimental import pallas as pl
from jax.experimental.pallas import tpu as pltpu
from jax.sharding import PartitionSpec as P

MESH = pl.DeviceIdType.MESH
PARTS = 4
LANES = 128
RELAYED = (3, 3)
DIRECT = (3, 3)
ORDER = ((0, 0), (1, 0), (0, 1), (1, 1), (1, 2), (1, 3))
TAKE = (3,)


def flip_bits(q, k, count):
    out, bit = 0, 1
    while bit < count:
        a, b = (q // bit) % 2, (k // bit) % 2
        out = out + bit * (a + b - 2 * a * b)
        bit *= 2
    return out


def kernel(
    n_dp, n_exp, experts, capacity,
    grad_hbm, ids_ref, hist_g_ref, hist_h_ref, weight_hbm,
    out_ref, best_ref,
    grad_ref, held, weight, send, send_rest, recv, recv_rest, rest_rows, slots, mine, peaks_in,
    grad_sem, weight_sem, send_sem, recv_sem, send_rest_sem, recv_rest_sem, peak_send_sem, peak_recv_sem,
):
    tokens = grad_ref.shape[0]
    main = send.shape[1]
    slices = n_exp // experts
    chips = n_exp // 2
    my_dp, me = lax.axis_index("dp"), lax.axis_index("expert")
    q0, c0 = me // 2, me % 2
    partner = q0 * 2 + 1 - c0
    own = me // slices
    grad_load = pltpu.make_async_copy(grad_hbm, grad_ref, grad_sem)
    grad_load.start()
    load = pltpu.make_async_copy(weight_hbm.at[0], weight, weight_sem)

    barrier = pltpu.get_barrier_semaphore()

    everyone = n_dp * n_exp
    here = my_dp * n_exp + me

    def greet(j, x):
        peer = (here + j) % everyone
        pl.semaphore_signal(
            barrier, inc=1, device_id=(peer // n_exp, peer % n_exp), device_id_type=MESH
        )
        return x

    lax.fori_loop(1, everyone, greet, 0)

    expert_row = lax.broadcasted_iota(jnp.int32, (LANES, tokens), 0)
    ids = ids_ref[...]
    mask_t = jnp.where((ids[0:1, :] == expert_row) | (ids[1:2, :] == expert_row), 1.0, 0.0)
    row = lax.broadcasted_iota(jnp.int32, (tokens, tokens), 0)
    col = lax.broadcasted_iota(jnp.int32, (tokens, tokens), 1)
    earlier = jnp.where(row < col, 1.0, 0.0).astype(jnp.bfloat16)
    before = jnp.dot(mask_t.astype(jnp.bfloat16), earlier, preferred_element_type=jnp.float32)
    slots[...] = jnp.where(mask_t > 0.5, before, -1.0)
    scale_in = 1.0 / jnp.max(hist_g_ref[...], axis=0, keepdims=True)
    scale_hidden = 1.0 / jnp.max(hist_h_ref[...], axis=0, keepdims=True)
    which = lax.broadcasted_iota(jnp.int32, (1, experts), 1)

    def pick(values, e):
        return jnp.sum(jnp.where(which == e, values, 0.0), axis=1, keepdims=True)

    position = lax.broadcasted_iota(jnp.int32, (capacity, tokens), 0).astype(jnp.float32)

    def prepare(e):
        onehot = jnp.where(slots[pl.ds(e, 1), :] == position, 1.0, 0.0).astype(jnp.bfloat16)
        rows = jnp.dot(onehot, grad_ref[...], preferred_element_type=jnp.float32)
        block = jnp.clip(rows * pick(scale_in, e), -1.0, 1.0)
        send[e] = block[0:main].astype(jnp.bfloat16)
        send_rest[e] = block[main:capacity].astype(jnp.bfloat16)

    span = weight.shape[1] // PARTS

    def outgoing(d, p):
        columns = pl.ds(p * span, span)
        return pltpu.make_async_remote_copy(
            src_ref=send.at[d // slices, :, columns], dst_ref=recv.at[me, :, columns],
            send_sem=send_sem.at[p, d], recv_sem=recv_sem.at[p, me],
            device_id=(my_dp, d), device_id_type=MESH,
        )

    def outgoing_rest(d):
        return pltpu.make_async_remote_copy(
            src_ref=send_rest.at[d // slices], dst_ref=recv_rest.at[me],
            send_sem=send_rest_sem.at[d], recv_sem=recv_rest_sem.at[me],
            device_id=(my_dp, d), device_id_type=MESH,
        )

    def incoming(s, p):
        columns = pl.ds(p * span, span)
        return pltpu.make_async_remote_copy(
            src_ref=send.at[0, :, columns], dst_ref=recv.at[s, :, columns],
            send_sem=send_sem.at[p, s], recv_sem=recv_sem.at[p, s],
            device_id=(my_dp, s), device_id_type=MESH,
        )

    def incoming_rest(s):
        return pltpu.make_async_remote_copy(
            src_ref=send_rest.at[0], dst_ref=recv_rest.at[s],
            send_sem=send_rest_sem.at[s], recv_sem=recv_rest_sem.at[s],
            device_id=(my_dp, s), device_id_type=MESH,
        )

    def chip_of(j):
        k = j
        if chips & (chips - 1) == 0:
            return flip_bits(q0, k, chips)
        return (q0 + k) % chips

    def source_of(j):
        if chips & (chips - 1) == 0:
            return chip_of(j)
        k = j
        return (q0 + chips - k) % chips

    def prepare_pair(q):
        prepare(2 * q + c0)
        prepare(2 * q + 1 - c0)

    def send_pair(q):
        for p in range(PARTS):
            for c in (c0, 1 - c0):
                outgoing(2 * q + c, p).start()
                if p == 0:
                    outgoing_rest(2 * q + c).start()

    greeted = everyone - 1
    grad_load.wait()
    load.start()
    if slices == 1:
        prepare_pair(chip_of(jnp.int32(1)))
        pl.semaphore_wait(barrier, greeted)

        def step(j, x):
            prepare_pair(chip_of((j + 1) % chips))
            send_pair(chip_of(j))
            return x
    else:
        def fill(e, x):
            prepare(e)
            return x

        lax.fori_loop(0, experts, fill, 0)
        pl.semaphore_wait(barrier, greeted)

        def step(j, x):
            send_pair(chip_of(j))
            return x

    lax.fori_loop(1, chips, step, 0)
    for p in range(PARTS):
        outgoing(partner, p).start()
    outgoing_rest(partner).start()

    recv[me] = send[own]
    recv_rest[me] = send_rest[own]
    row_peak = jnp.max(jnp.abs(grad_ref[...]).astype(jnp.float32), axis=1, keepdims=True)
    grad_peak = jnp.max(jnp.where(mask_t.T > 0.5, row_peak, 0.0), axis=0, keepdims=True)

    back = 1.0 / pick(scale_in, own)
    own_hidden = pick(scale_hidden, own)
    load.wait()

    def times_weight(block, columns):
        return lax.dot_general(
            block, weight[:, columns], (((1,), (1,)), ((), ())), preferred_element_type=jnp.float32
        )

    def multiply(block):
        return finish(times_weight(block, slice(None)))

    def finish(product):
        hidden = product * back
        scaled = jnp.clip(hidden * own_hidden, -1.0, 1.0)
        return scaled, jnp.max(jnp.max(jnp.abs(hidden), axis=0, keepdims=True), axis=1, keepdims=True)

    def pair_rows(q):
        return recv[pl.ds(2 * q, 2)].reshape(2 * main, recv.shape[2])

    def put_pair(q, scaled):
        for c in range(2):
            held[2 * q + c] = scaled[c * main:(c + 1) * main].astype(jnp.bfloat16)

    def take_own():
        for p in range(PARTS):
            incoming(partner, p).wait_recv()
        scaled, peak = multiply(pair_rows(q0))
        put_pair(q0, scaled)
        return peak

    def take(j, peak):
        q = source_of(j)
        for p in range(PARTS):
            incoming(2 * q, p).wait_recv()
            incoming(2 * q + 1, p).wait_recv()
        scaled, peak_here = multiply(pair_rows(q))
        put_pair(q, scaled)
        return jnp.maximum(peak, peak_here)

    peak = lax.fori_loop(1, chips - 1, take, take_own())

    def take_rest(j, x):
        incoming_rest((me + j) % n_exp).wait_recv()
        return x

    lax.fori_loop(1, n_exp, take_rest, 0)
    rest = capacity - main
    for s in range(n_exp):
        rest_rows[s * rest:(s + 1) * rest, :] = recv_rest[s].astype(jnp.float32)
    last = source_of(jnp.int32(chips - 1))
    product = None
    for p in range(PARTS):
        incoming(2 * last, p).wait_recv()
        incoming(2 * last + 1, p).wait_recv()
        columns = slice(p * span, (p + 1) * span)
        pair = recv[pl.ds(2 * last, 2), :, columns].reshape(2 * main, span)
        block = jnp.concatenate([pair, rest_rows[:, columns].astype(jnp.bfloat16)], axis=0)
        piece = times_weight(block, columns)
        product = piece if product is None else product + piece
    scaled, peak_here = finish(product)
    peak = jnp.maximum(peak, peak_here)

    at = lax.broadcasted_iota(jnp.int32, (1, LANES), 1)
    hidden_peak = jnp.where(at == own, peak, 0.0)
    part = lax.broadcasted_iota(jnp.int32, (8, LANES), 0)
    mine[...] = jnp.where(part == 0, grad_peak, jnp.where(part == 1, hidden_peak, 0.0))

    def peak_copy(peer, slot, j):
        return pltpu.make_async_remote_copy(
            src_ref=mine, dst_ref=peaks_in.at[slot],
            send_sem=peak_send_sem.at[j], recv_sem=peak_recv_sem.at[slot],
            device_id=(peer // n_exp, peer % n_exp), device_id_type=MESH,
        )

    def peak_start(j, x):
        peak_copy((here + j) % everyone, here, j).start()
        return x

    def peak_fold(j, best):
        peer = (here + j) % everyone
        peak_copy(peer, peer, j).wait_recv()
        return jnp.maximum(best, peaks_in[peer])

    def peak_finish(j, x):
        peak_copy((here + j) % everyone, here, j).wait_send()
        return x

    lax.fori_loop(1, everyone, peak_start, 0)
    put_pair(last, scaled)
    for s in range(n_exp):
        at_row = 2 * main + s * rest
        base = s * capacity
        out_ref[base:base + main, :] = held[s]
        out_ref[base + main:base + capacity, :] = scaled[at_row:at_row + rest].astype(jnp.bfloat16)
    best = lax.fori_loop(1, everyone, peak_fold, mine[...])
    lax.fori_loop(1, everyone, peak_finish, 0)

    best_ref[...] = best

    def drain(j, x):
        for p in range(PARTS):
            outgoing((me + j) % n_exp, p).wait_send()
        outgoing_rest((me + j) % n_exp).wait_send()
        return x

    lax.fori_loop(1, n_exp, drain, 0)


def finish_kernel(hist_g_ref, hist_h_ref, best_ref, out_ref, new_g_ref, new_h_ref, final_ref):
    final_ref[...] = out_ref[...]
    keep = hist_g_ref.shape[0] - 1
    experts = hist_g_ref.shape[1]
    new_g_ref[0:keep, :] = hist_g_ref[1:keep + 1, :]
    new_g_ref[keep:keep + 1, :] = best_ref[0:1, 0:experts]
    new_h_ref[0:keep, :] = hist_h_ref[1:keep + 1, :]
    new_h_ref[keep:keep + 1, :] = best_ref[1:2, 0:experts]


def by_blocks(grad_out, expert_ids, down_weight, history_grad, history_hidden):
    tokens, width = grad_out.shape
    experts = history_grad.shape[1]
    n_dp, n_exp = lax.axis_size("dp"), lax.axis_size("expert")
    capacity = tokens * 9 // 32
    main = (capacity - 1) // 16 * 16
    rest = capacity - main
    units = down_weight.shape[1]
    vmem = pl.BlockSpec(memory_space=pltpu.VMEM)
    dma = pltpu.SemaphoreType.DMA
    out, best = pl.pallas_call(
        functools.partial(kernel, n_dp, n_exp, experts, capacity),
        out_shape=(
            jax.ShapeDtypeStruct((n_exp * capacity, units), jnp.bfloat16),
            jax.ShapeDtypeStruct((8, LANES), jnp.float32),
        ),
        in_specs=[pl.BlockSpec(memory_space=pl.ANY), vmem, vmem, vmem, pl.BlockSpec(memory_space=pl.ANY)],
        out_specs=(vmem, vmem),
        scratch_shapes=[
            pltpu.VMEM((tokens, width), jnp.bfloat16),
            pltpu.VMEM((n_exp, main, units), jnp.bfloat16),
            pltpu.VMEM((units, width), jnp.bfloat16),
            pltpu.VMEM((experts, main, width), jnp.bfloat16),
            pltpu.VMEM((experts, rest, width), jnp.bfloat16),
            pltpu.VMEM((n_exp, main, width), jnp.bfloat16),
            pltpu.VMEM((n_exp, rest, width), jnp.bfloat16),
            pltpu.VMEM((n_exp * rest, width), jnp.float32),
            pltpu.VMEM((LANES, tokens), jnp.float32),
            pltpu.VMEM((8, LANES), jnp.float32),
            pltpu.VMEM((n_dp * n_exp, 8, LANES), jnp.float32),
            dma, dma, dma((PARTS, n_exp)), dma((PARTS, n_exp)), dma((n_exp,)), dma((n_exp,)),
            dma((n_dp * n_exp,)), dma((n_dp * n_exp,)),
        ],
        compiler_params=pltpu.CompilerParams(
            collective_id=0, has_side_effects=True, vmem_limit_bytes=60 * 1024 * 1024
        ),
    )(grad_out, expert_ids.T, history_grad, history_hidden, down_weight)
    new_g, new_h, out = pl.pallas_call(
        finish_kernel,
        out_shape=(
            jax.ShapeDtypeStruct(history_grad.shape, jnp.float32),
            jax.ShapeDtypeStruct(history_hidden.shape, jnp.float32),
            jax.ShapeDtypeStruct(out.shape, out.dtype),
        ),
        in_specs=[vmem, vmem, vmem, vmem],
        out_specs=(vmem, vmem, vmem),
    )(history_grad, history_hidden, best, out)
    return out.reshape(1, 1, n_exp * capacity, units), new_g, new_h


def chunk_edges(width):
    unit, edges = width // sum(RELAYED + DIRECT), [0]
    for pieces in RELAYED + DIRECT:
        edges.append(edges[-1] + pieces * unit)
    return edges


def relay_kernel(
    n_dp, n_exp, experts, capacity,
    grad_hbm, ids_hbm, hist_g_hbm, hist_h_hbm, weight_hbm,
    out_ref, best_ref,
    grad, ids_ref, hist_g_ref, hist_h_ref, raw, weight,
    send, send_rest, far, far_rest, relay, relay_rest, recv, recv_rest,
    counter, rest_rows, acc, slots, slots_in, onehot, mine, peaks_in,
    load_sem, known, slot_send, slot_recv, raw_send, raw_recv,
    near_send, far_send, relay_send,
    chunk_recv, peak_send, peak_recv,
):
    tokens, width = grad.shape
    main = send.shape[1]
    rest = capacity - main
    half, deep = n_exp // 2, n_exp // 4
    edges = chunk_edges(width)
    hops, chunks = len(RELAYED), len(edges) - 1
    relayed = edges[hops]
    my_dp, me = lax.axis_index("dp"), lax.axis_index("expert")
    q0, c0 = me // 2, me % 2
    side = q0 // deep
    base, far_base = side * half, (1 - side) * half
    my_i, my_k = me - base, q0 - side * deep
    inner = q0 == deep - 1 + side
    outer = jnp.logical_not(inner)
    partner = q0 * 2 + 1 - c0
    kind = jnp.where(inner, 0, 1)

    def seat_of(which):
        return half + c0 * deep + side + which - 2 * side * which

    across = 2 * (deep - side) + c0
    behind = 2 * (deep - 1 + side + jnp.where(inner, 2 * side - 1, 0)) + c0
    everyone = n_dp * n_exp
    here = my_dp * n_exp + me
    turn = me * n_dp + my_dp

    def loading(src, dst, at):
        return pltpu.make_async_copy(src, dst, load_sem.at[at])

    small = (
        loading(ids_hbm, ids_ref, 0), loading(hist_g_hbm, hist_g_ref, 1), loading(hist_h_hbm, hist_h_ref, 2)
    )
    grad_load = loading(grad_hbm, grad, 3)
    load = loading(weight_hbm.at[0], weight, 4)
    for copy in small:
        copy.start()
    grad_load.start()

    def tell(semaphore, d, dp=None):
        pl.semaphore_signal(
            semaphore, inc=1, device_id=(my_dp if dp is None else dp, d), device_id_type=MESH
        )

    barrier = pltpu.get_barrier_semaphore()

    @pl.when(inner)
    def _():
        tell(barrier, across)
        tell(barrier, behind)

    tell(barrier, partner)
    if n_dp in (2, 4):
        close = [flip_bits(my_dp, bit, n_dp) for bit in (1, 2) if bit < n_dp]
    else:
        close = [(my_dp + d) % n_dp for d in range(1, n_dp)]
    for d in close:
        tell(barrier, me, d)

    expert_row = lax.broadcasted_iota(jnp.int32, (LANES, tokens), 0)
    row = lax.broadcasted_iota(jnp.int32, (tokens, tokens), 0)
    col = lax.broadcasted_iota(jnp.int32, (tokens, tokens), 1)
    earlier = jnp.where(row < col, 1.0, 0.0).astype(jnp.bfloat16)
    for copy in small:
        copy.wait()
    ids = ids_ref[...]
    mask_t = jnp.where((ids[0:1, :] == expert_row) | (ids[1:2, :] == expert_row), 1.0, 0.0)
    before = jnp.dot(mask_t.astype(jnp.bfloat16), earlier, preferred_element_type=jnp.float32)
    slots[...] = jnp.where(mask_t > 0.5, before, -1.0)
    scale_in = 1.0 / jnp.max(hist_g_ref[...], axis=0, keepdims=True)
    scale_hidden = 1.0 / jnp.max(hist_h_ref[...], axis=0, keepdims=True)
    which = lax.broadcasted_iota(jnp.int32, (1, experts), 1)

    def pick(values, e):
        return jnp.sum(jnp.where(which == e, values, 0.0), axis=1, keepdims=True)

    position = lax.broadcasted_iota(jnp.int32, (main, tokens), 0).astype(jnp.float32)
    rest_row = lax.broadcasted_iota(jnp.int32, (half * rest, tokens), 0)
    rest_position = (rest_row % rest + main).astype(jnp.float32)
    rest_group = rest_row // rest

    def spread(at, slot_row, first):
        spare = jnp.full((half * rest, tokens), -1.0, jnp.float32)
        for i in range(half):
            named = slot_row(first + i)
            onehot[at, i * main:(i + 1) * main, :] = jnp.where(
                named == position, 1.0, 0.0
            ).astype(jnp.bfloat16)
            spare = jnp.where(rest_group == i, named, spare)
        onehot[at, half * main:half * capacity, :] = jnp.where(
            spare == rest_position, 1.0, 0.0
        ).astype(jnp.bfloat16)

    def own_row(e):
        return slots[pl.ds(e, 1), :]

    group_column = lax.broadcasted_iota(jnp.int32, (half * rest, 1), 0) // rest

    def scales_of(first):
        scales = [pick(scale_in, first + i) for i in range(half)]
        spare = jnp.zeros((half * rest, 1), jnp.float32)
        for i in range(half):
            spare = jnp.where(group_column == i, scales[i], spare)
        return scales, spare

    def fill(at, source, scales, put, put_rest):
        rows = jnp.dot(onehot[at], source, preferred_element_type=jnp.float32)
        each, spare = scales
        for i in range(half):
            put(i, jnp.clip(rows[i * main:(i + 1) * main] * each[i], -1.0, 1.0).astype(jnp.bfloat16))
        ends = jnp.clip(rows[half * main:half * capacity] * spare, -1.0, 1.0)
        for i in range(half):
            put_rest(i, ends[i * rest:(i + 1) * rest].astype(jnp.bfloat16))

    def columns_of(p, origin=0):
        return slice(edges[p] - origin, edges[p + 1] - origin)

    def remote(src, dst, send_sem, recv_sem, d):
        return pltpu.make_async_remote_copy(
            src_ref=src, dst_ref=dst, send_sem=send_sem, recv_sem=recv_sem,
            device_id=(my_dp, d), device_id_type=MESH,
        )

    def sent(ref, send_sem):
        remote(ref, ref, send_sem, send_sem, partner).wait_send()

    def came(ref, recv_sem):
        remote(ref, ref, recv_sem, recv_sem, partner).wait_recv()

    def send_raw(p):
        columns = columns_of(p)
        remote(
            grad.at[:, columns], raw.at[kind, :, columns], raw_send, raw_recv.at[kind * hops + p], across
        ).start()

    def send_slots():
        remote(
            slots.at[pl.ds(0, experts)], slots_in.at[kind], slot_send, slot_recv.at[kind], across
        ).start()

    def send_near(p):
        columns = columns_of(p)
        for j in range(1, half):
            i = (my_i + j) % half
            remote(
                send.at[i, :, columns], recv.at[my_i, :, columns], near_send, chunk_recv.at[p], base + i
            ).start()
            remote(
                send_rest.at[i, :, columns], recv_rest.at[my_i, :, columns],
                near_send, chunk_recv.at[p], base + i,
            ).start()

    outside = 2 * (1 - side)
    outside_first = ((outside + c0, outside + 1 - c0), (half - 2 - outside + c0, half - 1 - outside - c0))

    def send_far(p, targets):
        columns, at = columns_of(p), half + c0 * deep + my_k
        for i in targets:
            remote(
                far.at[i, :, columns_of(p, relayed)], recv.at[at, :, columns],
                far_send, chunk_recv.at[p], far_base + i,
            ).start()

    def send_far_rest(targets):
        columns, at = pl.ds(relayed, width - relayed), half + c0 * deep + my_k
        for i in targets:
            remote(
                far_rest.at[i], recv_rest.at[at, :, columns],
                far_send, chunk_recv.at[hops], far_base + i,
            ).start()

    def send_relay(which, p):
        columns = columns_of(p)
        for j in range(1, half):
            i = (my_i + j) % half
            remote(
                relay.at[i, which, :, columns], recv.at[seat_of(which), :, columns],
                relay_send, chunk_recv.at[p], base + i,
            ).start()
            remote(
                relay_rest.at[i, which, :, columns], recv_rest.at[seat_of(which), :, columns],
                relay_send, chunk_recv.at[p], base + i,
            ).start()

    def wait_chunk(p, senders):
        size = edges[p + 1] - edges[p]
        blocks = senders * size // rest * capacity
        if p == hops:
            blocks += 2 * (width - relayed - size)
        elif p > hops:
            blocks -= 2 * size
        came(counter.at[:, 0:blocks], chunk_recv.at[p])

    spread(0, own_row, base)
    spread(1, own_row, far_base)
    near_scales = scales_of(base)
    grad_load.wait()
    load.start()
    pl.semaphore_wait(barrier, 2 + len(close))
    tell(known.at[0], partner)

    @pl.when(inner)
    def _():
        tell(known.at[0], across)
        send_slots()

        for p in range(hops):
            send_raw(p)
        pl.semaphore_wait(known.at[0], 3)
        tell(known.at[1], across)
        tell(known.at[1], behind)

    @pl.when(outer)
    def _():
        tell(known.at[0], behind)
        pl.semaphore_wait(known.at[0], 1)

    for d in close:
        tell(known.at[2], me, d)

    def direct(p):
        columns = columns_of(p)

        def put(i, block):
            send[i, :, columns] = block

        def put_rest(i, block):
            send_rest[i, :, columns] = block

        fill(0, grad[:, columns], near_scales, put, put_rest)
        send_near(p)

        if p == 1:
            pl.semaphore_wait(known.at[1], 1)
            if close:
                pl.semaphore_wait(known.at[2], len(close))

            @pl.when(outer)
            def _():
                send_slots()

        @pl.when(outer)
        def _():
            if p > 0:
                send_raw(p - 1)
            if p == chunks - 1:
                send_raw(p)

    for p in range(chunks):
        direct(p)

    def fill_far(p):
        columns = columns_of(p, relayed)

        def put(i, block):
            far[i, :, columns] = block

        def put_rest(i, block):
            far_rest[i, :, columns] = block

        fill(1, grad[:, columns_of(p)], far_scales, put, put_rest)

    far_scales = scales_of(far_base)

    @pl.when(inner)
    def _():
        for p in range(hops, chunks):
            fill_far(p)
        for targets in outside_first:
            send_far_rest(targets)
            for p in range(hops, chunks):
                send_far(p, targets)

    recv[my_i] = send[my_i]
    recv_rest[my_i] = send_rest[my_i]
    row_peak = jnp.max(jnp.abs(grad[...]).astype(jnp.float32), axis=1, keepdims=True)
    grad_peak = jnp.max(jnp.where(mask_t.T > 0.5, row_peak, 0.0), axis=0, keepdims=True)
    back = 1.0 / pick(scale_in, me)
    own_hidden = pick(scale_hidden, me)

    load.wait()

    def add_product(p, first=False):
        columns, size = columns_of(p), edges[p + 1] - edges[p]
        for s in range(n_exp):
            rest_rows[s * rest:(s + 1) * rest, 0:size] = recv_rest[s, :, columns].astype(jnp.float32)
        block = jnp.concatenate(
            [
                recv[:, :, columns].reshape(n_exp * main, size),
                rest_rows[:, 0:size].astype(jnp.bfloat16),
            ],
            axis=0,
        )
        product = lax.dot_general(
            block, weight[:, columns], (((1,), (1,)), ((), ())), preferred_element_type=jnp.float32
        )
        acc[...] = product if first else acc[...] + product

    def get_ready(which):
        @pl.when(inner)
        def _():
            came(slots_in.at[which], slot_recv.at[which])
            spread(2 + which, lambda e: slots_in[which, pl.ds(e, 1), :], base)

    def pass_on(which, p):
        columns = columns_of(p)

        @pl.when(inner)
        def _():
            came(raw.at[which, :, columns], raw_recv.at[which * hops + p])

            def put(i, block):
                relay[i, which, :, columns] = block

            def put_rest(i, block):
                relay_rest[i, which, :, columns] = block

            fill(2 + which, raw[which, :, columns], near_scales, put, put_rest)
            send_relay(which, p)
            recv[seat_of(which), :, columns] = relay[my_i, which, :, columns]
            recv_rest[seat_of(which), :, columns] = relay_rest[my_i, which, :, columns]

    def multiply(p):
        @pl.when(inner)
        def _():
            wait_chunk(p, half - 1 + deep if p < hops else n_exp - 2)

        @pl.when(outer)
        def _():
            wait_chunk(p, n_exp - 1)

        add_product(p, p == 0)

    for at, (which, p) in enumerate(ORDER):
        if p == 0:
            get_ready(which)
        pass_on(which, p)
        for taken, place in enumerate(TAKE):
            if place == at:
                multiply(taken)
    for p in range(len(TAKE), chunks):
        multiply(p)
    hidden = acc[...] * back
    peak = jnp.max(jnp.max(jnp.abs(hidden), axis=0, keepdims=True), axis=1, keepdims=True)
    lane = lax.broadcasted_iota(jnp.int32, (1, LANES), 1)
    mine[...] = jnp.where(lane < experts, grad_peak, jnp.where(lane == experts + me, peak, 0.0))
    for j in range(everyone - 1):
        peer = jnp.where(j >= turn, j + 1, j)
        pltpu.make_async_remote_copy(
            src_ref=mine, dst_ref=peaks_in.at[here], send_sem=peak_send, recv_sem=peak_recv,
            device_id=(peer % n_dp, peer // n_dp), device_id_type=MESH,
        ).start()
    peaks_in[here] = mine[...]
    scaled = jnp.clip(acc[...] * back * own_hidden, -1.0, 1.0)
    for at in range(n_exp):
        if at < half:
            block, first = side, at * capacity
        else:
            block, first = 1 - side, ((at - half) % deep * 2 + (at - half) // deep) * capacity
        out_ref[block, first:first + main, :] = scaled[at * main:(at + 1) * main].astype(jnp.bfloat16)
        tail = n_exp * main + at * rest
        out_ref[block, first + main:first + capacity, :] = scaled[tail:tail + rest].astype(jnp.bfloat16)

    per_block = capacity // rest
    sent(slots.at[pl.ds(0, experts)], slot_send)
    sent(counter.at[:, 0:(half - 1) * per_block * width], near_send)

    @pl.when(outer)
    def _():
        sent(grad, raw_send)

    @pl.when(inner)
    def _():
        sent(grad.at[:, pl.ds(0, relayed)], raw_send)
        sent(counter.at[:, 0:half * per_block * (width - relayed)], far_send)
        sent(counter.at[:, 0:(half - 1) * per_block * (relayed + width)], relay_send)

    others = peaks_in.at[pl.ds(0, everyone - 1)]
    sent(others, peak_send)
    came(others, peak_recv)
    best_ref[...] = jnp.max(peaks_in[...], axis=0)


def relay_finish(
    hist_g_ref, hist_h_ref, best_ref, out_ref, new_g_hbm, new_h_hbm, final_hbm, new_g, new_h, sem
):
    result = pltpu.make_async_copy(out_ref, final_hbm, sem.at[0])
    result.start()
    keep = hist_g_ref.shape[0] - 1
    experts = hist_g_ref.shape[1]
    new_g[0:keep, :] = hist_g_ref[1:keep + 1, :]
    new_g[keep:keep + 1, :] = best_ref[0:1, 0:experts]
    new_h[0:keep, :] = hist_h_ref[1:keep + 1, :]
    new_h[keep:keep + 1, :] = best_ref[0:1, experts:2 * experts]
    first = pltpu.make_async_copy(new_g, new_g_hbm, sem.at[1])
    second = pltpu.make_async_copy(new_h, new_h_hbm, sem.at[2])
    first.start()
    second.start()
    first.wait()
    second.wait()
    result.wait()


def by_relay(grad_out, expert_ids, down_weight, history_grad, history_hidden):
    tokens, width = grad_out.shape
    experts = history_grad.shape[1]
    n_dp, n_exp = lax.axis_size("dp"), lax.axis_size("expert")
    capacity = tokens * 9 // 32
    main = (capacity - 1) // 16 * 16
    rest = capacity - main
    units = down_weight.shape[1]
    half, deep = n_exp // 2, n_exp // 4
    edges = chunk_edges(width)
    chunks, hops = len(edges) - 1, len(RELAYED)
    span = max(after - before for before, after in zip(edges, edges[1:]))
    tail = width - edges[hops]
    everyone = n_dp * n_exp
    vmem, anywhere = pl.BlockSpec(memory_space=pltpu.VMEM), pl.BlockSpec(memory_space=pl.ANY)
    dma = pltpu.SemaphoreType.DMA
    bf16, f32 = jnp.bfloat16, jnp.float32
    out, best = pl.pallas_call(
        functools.partial(relay_kernel, n_dp, n_exp, experts, capacity),
        out_shape=(pltpu.VMEM((2, half * capacity, units), bf16), pltpu.VMEM((1, LANES), f32)),
        in_specs=[anywhere] * 5,
        out_specs=(vmem, vmem),
        scratch_shapes=[
            pltpu.VMEM((tokens, width), bf16),
            pltpu.VMEM(expert_ids.shape[::-1], jnp.int32),
            pltpu.VMEM(history_grad.shape, f32),
            pltpu.VMEM(history_hidden.shape, f32),
            pltpu.VMEM((deep, tokens, width), bf16),
            pltpu.VMEM((units, width), bf16),
            pltpu.VMEM((half, main, width), bf16),
            pltpu.VMEM((half, rest, width), bf16),
            pltpu.VMEM((half, main, tail), bf16),
            pltpu.VMEM((half, rest, tail), bf16),
            pltpu.VMEM((half, deep, main, width), bf16),
            pltpu.VMEM((half, deep, rest, width), bf16),
            pltpu.VMEM((n_exp, main, width), bf16),
            pltpu.VMEM((n_exp, rest, width), bf16),
            pltpu.VMEM((rest, 2 * half * capacity // rest * width), bf16),
            pltpu.VMEM((n_exp * rest, span), f32),
            pltpu.VMEM((n_exp * capacity, units), f32),
            pltpu.VMEM((LANES, tokens), f32),
            pltpu.VMEM((deep, experts, tokens), f32),
            pltpu.VMEM((2 + deep, half * capacity, tokens), bf16),
            pltpu.VMEM((1, LANES), f32),
            pltpu.VMEM((everyone, 1, LANES), f32),
            dma((5,)), pltpu.SemaphoreType.REGULAR((3,)), dma, dma((deep,)), dma, dma((hops + chunks,)),
            dma, dma, dma,
            dma((chunks,)), dma, dma,
        ],
        compiler_params=pltpu.CompilerParams(
            collective_id=1, has_side_effects=True, vmem_limit_bytes=56 * 1024 * 1024
        ),
    )(grad_out, expert_ids.T, history_grad, history_hidden, down_weight)
    new_g, new_h, out = pl.pallas_call(
        relay_finish,
        out_shape=(
            jax.ShapeDtypeStruct(history_grad.shape, f32),
            jax.ShapeDtypeStruct(history_hidden.shape, f32),
            jax.ShapeDtypeStruct((2, half * capacity, units), bf16),
        ),
        in_specs=[vmem, vmem, vmem, vmem],
        out_specs=(anywhere, anywhere, anywhere),
        scratch_shapes=[
            pltpu.VMEM(history_grad.shape, f32), pltpu.VMEM(history_hidden.shape, f32), dma((3,))
        ],
        compiler_params=pltpu.CompilerParams(vmem_limit_bytes=4 * 1024 * 1024),
    )(history_grad, history_hidden, best, out)
    return out.reshape(1, 1, n_exp * capacity, units), new_g, new_h


def fits_relay(tokens, width, experts, n_exp):
    capacity = tokens * 9 // 32
    return (
        experts == n_exp and n_exp // 4 == 2 and experts % 8 == 0 and 2 * experts <= LANES
        and tokens % LANES == 0 and width % (sum(RELAYED + DIRECT) * LANES) == 0
        and (n_exp // 2 * capacity) % 16 == 0 and (n_exp // 2 * (capacity % 16)) % 16 == 0
        and 0 < capacity % 16 and capacity % (capacity % 16) == 0
    )


def per_device(*arguments):
    (tokens, width), experts = arguments[0].shape, arguments[3].shape[1]
    if fits_relay(tokens, width, experts, lax.axis_size("expert")):
        return by_relay(*arguments)
    return by_blocks(*arguments)


def solution(mesh):
    in_specs = (
        P(("dp", "expert"), None),
        P(("dp", "expert"), None),
        P("expert", None, None),
        P(),
        P(),
    )
    out_specs = (P("dp", "expert", None, None), P(), P())
    return jax.shard_map(
        per_device, mesh=mesh, in_specs=in_specs, out_specs=out_specs, check_vma=False
    )
```

```python
import functools

import jax
import jax.numpy as jnp
from jax import lax
from jax.experimental import pallas as pl
from jax.experimental.pallas import tpu as pltpu
from jax.sharding import PartitionSpec as P

MESH = pl.DeviceIdType.MESH
PARTS = 4
LANES = 128
RELAYED = (3, 3, 1)
DIRECT = (3, 2)
ORDER = ((0, 0), (1, 0), (0, 1), (1, 1), (1, 2), (1, 3), (0, 2), (1, 4))
TAKE = (3,)


def flip_bits(q, k, count):
    out, bit = 0, 1
    while bit < count:
        a, b = (q // bit) % 2, (k // bit) % 2
        out = out + bit * (a + b - 2 * a * b)
        bit *= 2
    return out


def kernel(
    n_dp, n_exp, experts, capacity,
    grad_hbm, ids_ref, hist_g_ref, hist_h_ref, weight_hbm,
    out_ref, best_ref,
    grad_ref, held, weight, send, send_rest, recv, recv_rest, rest_rows, slots, mine, peaks_in,
    grad_sem, weight_sem, send_sem, recv_sem, send_rest_sem, recv_rest_sem, peak_send_sem, peak_recv_sem,
):
    tokens = grad_ref.shape[0]
    main = send.shape[1]
    slices = n_exp // experts
    chips = n_exp // 2
    my_dp, me = lax.axis_index("dp"), lax.axis_index("expert")
    q0, c0 = me // 2, me % 2
    partner = q0 * 2 + 1 - c0
    own = me // slices
    grad_load = pltpu.make_async_copy(grad_hbm, grad_ref, grad_sem)
    grad_load.start()
    load = pltpu.make_async_copy(weight_hbm.at[0], weight, weight_sem)

    barrier = pltpu.get_barrier_semaphore()

    everyone = n_dp * n_exp
    here = my_dp * n_exp + me

    def greet(j, x):
        peer = (here + j) % everyone
        pl.semaphore_signal(
            barrier, inc=1, device_id=(peer // n_exp, peer % n_exp), device_id_type=MESH
        )
        return x

    lax.fori_loop(1, everyone, greet, 0)

    expert_row = lax.broadcasted_iota(jnp.int32, (LANES, tokens), 0)
    ids = ids_ref[...]
    mask_t = jnp.where((ids[0:1, :] == expert_row) | (ids[1:2, :] == expert_row), 1.0, 0.0)
    row = lax.broadcasted_iota(jnp.int32, (tokens, tokens), 0)
    col = lax.broadcasted_iota(jnp.int32, (tokens, tokens), 1)
    earlier = jnp.where(row < col, 1.0, 0.0).astype(jnp.bfloat16)
    before = jnp.dot(mask_t.astype(jnp.bfloat16), earlier, preferred_element_type=jnp.float32)
    slots[...] = jnp.where(mask_t > 0.5, before, -1.0)
    scale_in = 1.0 / jnp.max(hist_g_ref[...], axis=0, keepdims=True)
    scale_hidden = 1.0 / jnp.max(hist_h_ref[...], axis=0, keepdims=True)
    which = lax.broadcasted_iota(jnp.int32, (1, experts), 1)

    def pick(values, e):
        return jnp.sum(jnp.where(which == e, values, 0.0), axis=1, keepdims=True)

    position = lax.broadcasted_iota(jnp.int32, (capacity, tokens), 0).astype(jnp.float32)

    def prepare(e):
        onehot = jnp.where(slots[pl.ds(e, 1), :] == position, 1.0, 0.0).astype(jnp.bfloat16)
        rows = jnp.dot(onehot, grad_ref[...], preferred_element_type=jnp.float32)
        block = jnp.clip(rows * pick(scale_in, e), -1.0, 1.0)
        send[e] = block[0:main].astype(jnp.bfloat16)
        send_rest[e] = block[main:capacity].astype(jnp.bfloat16)

    span = weight.shape[1] // PARTS

    def outgoing(d, p):
        columns = pl.ds(p * span, span)
        return pltpu.make_async_remote_copy(
            src_ref=send.at[d // slices, :, columns], dst_ref=recv.at[me, :, columns],
            send_sem=send_sem.at[p, d], recv_sem=recv_sem.at[p, me],
            device_id=(my_dp, d), device_id_type=MESH,
        )

    def outgoing_rest(d):
        return pltpu.make_async_remote_copy(
            src_ref=send_rest.at[d // slices], dst_ref=recv_rest.at[me],
            send_sem=send_rest_sem.at[d], recv_sem=recv_rest_sem.at[me],
            device_id=(my_dp, d), device_id_type=MESH,
        )

    def incoming(s, p):
        columns = pl.ds(p * span, span)
        return pltpu.make_async_remote_copy(
            src_ref=send.at[0, :, columns], dst_ref=recv.at[s, :, columns],
            send_sem=send_sem.at[p, s], recv_sem=recv_sem.at[p, s],
            device_id=(my_dp, s), device_id_type=MESH,
        )

    def incoming_rest(s):
        return pltpu.make_async_remote_copy(
            src_ref=send_rest.at[0], dst_ref=recv_rest.at[s],
            send_sem=send_rest_sem.at[s], recv_sem=recv_rest_sem.at[s],
            device_id=(my_dp, s), device_id_type=MESH,
        )

    def chip_of(j):
        k = j
        if chips & (chips - 1) == 0:
            return flip_bits(q0, k, chips)
        return (q0 + k) % chips

    def source_of(j):
        if chips & (chips - 1) == 0:
            return chip_of(j)
        k = j
        return (q0 + chips - k) % chips

    def prepare_pair(q):
        prepare(2 * q + c0)
        prepare(2 * q + 1 - c0)

    def send_pair(q):
        for p in range(PARTS):
            for c in (c0, 1 - c0):
                outgoing(2 * q + c, p).start()
                if p == 0:
                    outgoing_rest(2 * q + c).start()

    greeted = everyone - 1
    grad_load.wait()
    load.start()
    if slices == 1:
        prepare_pair(chip_of(jnp.int32(1)))
        pl.semaphore_wait(barrier, greeted)

        def step(j, x):
            prepare_pair(chip_of((j + 1) % chips))
            send_pair(chip_of(j))
            return x
    else:
        def fill(e, x):
            prepare(e)
            return x

        lax.fori_loop(0, experts, fill, 0)
        pl.semaphore_wait(barrier, greeted)

        def step(j, x):
            send_pair(chip_of(j))
            return x

    lax.fori_loop(1, chips, step, 0)
    for p in range(PARTS):
        outgoing(partner, p).start()
    outgoing_rest(partner).start()

    recv[me] = send[own]
    recv_rest[me] = send_rest[own]
    row_peak = jnp.max(jnp.abs(grad_ref[...]).astype(jnp.float32), axis=1, keepdims=True)
    grad_peak = jnp.max(jnp.where(mask_t.T > 0.5, row_peak, 0.0), axis=0, keepdims=True)

    back = 1.0 / pick(scale_in, own)
    own_hidden = pick(scale_hidden, own)
    load.wait()

    def times_weight(block, columns):
        return lax.dot_general(
            block, weight[:, columns], (((1,), (1,)), ((), ())), preferred_element_type=jnp.float32
        )

    def multiply(block):
        return finish(times_weight(block, slice(None)))

    def finish(product):
        hidden = product * back
        scaled = jnp.clip(hidden * own_hidden, -1.0, 1.0)
        return scaled, jnp.max(jnp.max(jnp.abs(hidden), axis=0, keepdims=True), axis=1, keepdims=True)

    def pair_rows(q):
        return recv[pl.ds(2 * q, 2)].reshape(2 * main, recv.shape[2])

    def put_pair(q, scaled):
        for c in range(2):
            held[2 * q + c] = scaled[c * main:(c + 1) * main].astype(jnp.bfloat16)

    def take_own():
        for p in range(PARTS):
            incoming(partner, p).wait_recv()
        scaled, peak = multiply(pair_rows(q0))
        put_pair(q0, scaled)
        return peak

    def take(j, peak):
        q = source_of(j)
        for p in range(PARTS):
            incoming(2 * q, p).wait_recv()
            incoming(2 * q + 1, p).wait_recv()
        scaled, peak_here = multiply(pair_rows(q))
        put_pair(q, scaled)
        return jnp.maximum(peak, peak_here)

    peak = lax.fori_loop(1, chips - 1, take, take_own())

    def take_rest(j, x):
        incoming_rest((me + j) % n_exp).wait_recv()
        return x

    lax.fori_loop(1, n_exp, take_rest, 0)
    rest = capacity - main
    for s in range(n_exp):
        rest_rows[s * rest:(s + 1) * rest, :] = recv_rest[s].astype(jnp.float32)
    last = source_of(jnp.int32(chips - 1))
    product = None
    for p in range(PARTS):
        incoming(2 * last, p).wait_recv()
        incoming(2 * last + 1, p).wait_recv()
        columns = slice(p * span, (p + 1) * span)
        pair = recv[pl.ds(2 * last, 2), :, columns].reshape(2 * main, span)
        block = jnp.concatenate([pair, rest_rows[:, columns].astype(jnp.bfloat16)], axis=0)
        piece = times_weight(block, columns)
        product = piece if product is None else product + piece
    scaled, peak_here = finish(product)
    peak = jnp.maximum(peak, peak_here)

    at = lax.broadcasted_iota(jnp.int32, (1, LANES), 1)
    hidden_peak = jnp.where(at == own, peak, 0.0)
    part = lax.broadcasted_iota(jnp.int32, (8, LANES), 0)
    mine[...] = jnp.where(part == 0, grad_peak, jnp.where(part == 1, hidden_peak, 0.0))

    def peak_copy(peer, slot, j):
        return pltpu.make_async_remote_copy(
            src_ref=mine, dst_ref=peaks_in.at[slot],
            send_sem=peak_send_sem.at[j], recv_sem=peak_recv_sem.at[slot],
            device_id=(peer // n_exp, peer % n_exp), device_id_type=MESH,
        )

    def peak_start(j, x):
        peak_copy((here + j) % everyone, here, j).start()
        return x

    def peak_fold(j, best):
        peer = (here + j) % everyone
        peak_copy(peer, peer, j).wait_recv()
        return jnp.maximum(best, peaks_in[peer])

    def peak_finish(j, x):
        peak_copy((here + j) % everyone, here, j).wait_send()
        return x

    lax.fori_loop(1, everyone, peak_start, 0)
    put_pair(last, scaled)
    for s in range(n_exp):
        at_row = 2 * main + s * rest
        base = s * capacity
        out_ref[base:base + main, :] = held[s]
        out_ref[base + main:base + capacity, :] = scaled[at_row:at_row + rest].astype(jnp.bfloat16)
    best = lax.fori_loop(1, everyone, peak_fold, mine[...])
    lax.fori_loop(1, everyone, peak_finish, 0)

    best_ref[...] = best

    def drain(j, x):
        for p in range(PARTS):
            outgoing((me + j) % n_exp, p).wait_send()
        outgoing_rest((me + j) % n_exp).wait_send()
        return x

    lax.fori_loop(1, n_exp, drain, 0)


def finish_kernel(hist_g_ref, hist_h_ref, best_ref, out_ref, new_g_ref, new_h_ref, final_ref):
    final_ref[...] = out_ref[...]
    keep = hist_g_ref.shape[0] - 1
    experts = hist_g_ref.shape[1]
    new_g_ref[0:keep, :] = hist_g_ref[1:keep + 1, :]
    new_g_ref[keep:keep + 1, :] = best_ref[0:1, 0:experts]
    new_h_ref[0:keep, :] = hist_h_ref[1:keep + 1, :]
    new_h_ref[keep:keep + 1, :] = best_ref[1:2, 0:experts]


def by_blocks(grad_out, expert_ids, down_weight, history_grad, history_hidden):
    tokens, width = grad_out.shape
    experts = history_grad.shape[1]
    n_dp, n_exp = lax.axis_size("dp"), lax.axis_size("expert")
    capacity = tokens * 9 // 32
    main = (capacity - 1) // 16 * 16
    rest = capacity - main
    units = down_weight.shape[1]
    vmem = pl.BlockSpec(memory_space=pltpu.VMEM)
    dma = pltpu.SemaphoreType.DMA
    out, best = pl.pallas_call(
        functools.partial(kernel, n_dp, n_exp, experts, capacity),
        out_shape=(
            jax.ShapeDtypeStruct((n_exp * capacity, units), jnp.bfloat16),
            jax.ShapeDtypeStruct((8, LANES), jnp.float32),
        ),
        in_specs=[pl.BlockSpec(memory_space=pl.ANY), vmem, vmem, vmem, pl.BlockSpec(memory_space=pl.ANY)],
        out_specs=(vmem, vmem),
        scratch_shapes=[
            pltpu.VMEM((tokens, width), jnp.bfloat16),
            pltpu.VMEM((n_exp, main, units), jnp.bfloat16),
            pltpu.VMEM((units, width), jnp.bfloat16),
            pltpu.VMEM((experts, main, width), jnp.bfloat16),
            pltpu.VMEM((experts, rest, width), jnp.bfloat16),
            pltpu.VMEM((n_exp, main, width), jnp.bfloat16),
            pltpu.VMEM((n_exp, rest, width), jnp.bfloat16),
            pltpu.VMEM((n_exp * rest, width), jnp.float32),
            pltpu.VMEM((LANES, tokens), jnp.float32),
            pltpu.VMEM((8, LANES), jnp.float32),
            pltpu.VMEM((n_dp * n_exp, 8, LANES), jnp.float32),
            dma, dma, dma((PARTS, n_exp)), dma((PARTS, n_exp)), dma((n_exp,)), dma((n_exp,)),
            dma((n_dp * n_exp,)), dma((n_dp * n_exp,)),
        ],
        compiler_params=pltpu.CompilerParams(
            collective_id=0, has_side_effects=True, vmem_limit_bytes=60 * 1024 * 1024
        ),
    )(grad_out, expert_ids.T, history_grad, history_hidden, down_weight)
    new_g, new_h, out = pl.pallas_call(
        finish_kernel,
        out_shape=(
            jax.ShapeDtypeStruct(history_grad.shape, jnp.float32),
            jax.ShapeDtypeStruct(history_hidden.shape, jnp.float32),
            jax.ShapeDtypeStruct(out.shape, out.dtype),
        ),
        in_specs=[vmem, vmem, vmem, vmem],
        out_specs=(vmem, vmem, vmem),
    )(history_grad, history_hidden, best, out)
    return out.reshape(1, 1, n_exp * capacity, units), new_g, new_h


def chunk_edges(width):
    unit, edges = width // sum(RELAYED + DIRECT), [0]
    for pieces in RELAYED + DIRECT:
        edges.append(edges[-1] + pieces * unit)
    return edges


def relay_kernel(
    n_dp, n_exp, experts, capacity,
    grad_hbm, ids_hbm, hist_g_hbm, hist_h_hbm, weight_hbm,
    out_ref, best_ref,
    grad, ids_ref, hist_g_ref, hist_h_ref, raw, weight,
    send, send_rest, far, far_rest, relay, relay_rest, recv, recv_rest,
    counter, rest_rows, acc, slots, slots_in, onehot, mine, peaks_in,
    load_sem, known, slot_send, slot_recv, raw_send, raw_recv,
    near_send, far_send, relay_send,
    chunk_recv, peak_send, peak_recv,
):
    tokens, width = grad.shape
    main = send.shape[1]
    rest = capacity - main
    half, deep = n_exp // 2, n_exp // 4
    edges = chunk_edges(width)
    hops, chunks = len(RELAYED), len(edges) - 1
    relayed = edges[hops]
    my_dp, me = lax.axis_index("dp"), lax.axis_index("expert")
    q0, c0 = me // 2, me % 2
    side = q0 // deep
    base, far_base = side * half, (1 - side) * half
    my_i, my_k = me - base, q0 - side * deep
    inner = q0 == deep - 1 + side
    outer = jnp.logical_not(inner)
    partner = q0 * 2 + 1 - c0
    kind = jnp.where(inner, 0, 1)

    def seat_of(which):
        return half + c0 * deep + side + which - 2 * side * which

    across = 2 * (deep - side) + c0
    behind = 2 * (deep - 1 + side + jnp.where(inner, 2 * side - 1, 0)) + c0
    everyone = n_dp * n_exp
    here = my_dp * n_exp + me
    turn = me * n_dp + my_dp

    def loading(src, dst, at):
        return pltpu.make_async_copy(src, dst, load_sem.at[at])

    small = (
        loading(ids_hbm, ids_ref, 0), loading(hist_g_hbm, hist_g_ref, 1), loading(hist_h_hbm, hist_h_ref, 2)
    )
    grad_load = loading(grad_hbm, grad, 3)
    load = loading(weight_hbm.at[0], weight, 4)
    for copy in small:
        copy.start()
    grad_load.start()

    def tell(semaphore, d, dp=None):
        pl.semaphore_signal(
            semaphore, inc=1, device_id=(my_dp if dp is None else dp, d), device_id_type=MESH
        )

    barrier = pltpu.get_barrier_semaphore()

    @pl.when(inner)
    def _():
        tell(barrier, across)
        tell(barrier, behind)

    tell(barrier, partner)
    if n_dp in (2, 4):
        close = [flip_bits(my_dp, bit, n_dp) for bit in (1, 2) if bit < n_dp]
    else:
        close = [(my_dp + d) % n_dp for d in range(1, n_dp)]
    for d in close:
        tell(barrier, me, d)

    expert_row = lax.broadcasted_iota(jnp.int32, (LANES, tokens), 0)
    row = lax.broadcasted_iota(jnp.int32, (tokens, tokens), 0)
    col = lax.broadcasted_iota(jnp.int32, (tokens, tokens), 1)
    earlier = jnp.where(row < col, 1.0, 0.0).astype(jnp.bfloat16)
    for copy in small:
        copy.wait()
    ids = ids_ref[...]
    mask_t = jnp.where((ids[0:1, :] == expert_row) | (ids[1:2, :] == expert_row), 1.0, 0.0)
    before = jnp.dot(mask_t.astype(jnp.bfloat16), earlier, preferred_element_type=jnp.float32)
    slots[...] = jnp.where(mask_t > 0.5, before, -1.0)
    scale_in = 1.0 / jnp.max(hist_g_ref[...], axis=0, keepdims=True)
    scale_hidden = 1.0 / jnp.max(hist_h_ref[...], axis=0, keepdims=True)
    which = lax.broadcasted_iota(jnp.int32, (1, experts), 1)

    def pick(values, e):
        return jnp.sum(jnp.where(which == e, values, 0.0), axis=1, keepdims=True)

    position = lax.broadcasted_iota(jnp.int32, (main, tokens), 0).astype(jnp.float32)
    rest_row = lax.broadcasted_iota(jnp.int32, (half * rest, tokens), 0)
    rest_position = (rest_row % rest + main).astype(jnp.float32)
    rest_group = rest_row // rest

    def spread(at, slot_row, first):
        spare = jnp.full((half * rest, tokens), -1.0, jnp.float32)
        for i in range(half):
            named = slot_row(first + i)
            onehot[at, i * main:(i + 1) * main, :] = jnp.where(
                named == position, 1.0, 0.0
            ).astype(jnp.bfloat16)
            spare = jnp.where(rest_group == i, named, spare)
        onehot[at, half * main:half * capacity, :] = jnp.where(
            spare == rest_position, 1.0, 0.0
        ).astype(jnp.bfloat16)

    def own_row(e):
        return slots[pl.ds(e, 1), :]

    group_column = lax.broadcasted_iota(jnp.int32, (half * rest, 1), 0) // rest

    def scales_of(first):
        scales = [pick(scale_in, first + i) for i in range(half)]
        spare = jnp.zeros((half * rest, 1), jnp.float32)
        for i in range(half):
            spare = jnp.where(group_column == i, scales[i], spare)
        return scales, spare

    def fill(at, source, scales, put, put_rest):
        rows = jnp.dot(onehot[at], source, preferred_element_type=jnp.float32)
        each, spare = scales
        for i in range(half):
            put(i, jnp.clip(rows[i * main:(i + 1) * main] * each[i], -1.0, 1.0).astype(jnp.bfloat16))
        ends = jnp.clip(rows[half * main:half * capacity] * spare, -1.0, 1.0)
        for i in range(half):
            put_rest(i, ends[i * rest:(i + 1) * rest].astype(jnp.bfloat16))

    def columns_of(p, origin=0):
        return slice(edges[p] - origin, edges[p + 1] - origin)

    def remote(src, dst, send_sem, recv_sem, d):
        return pltpu.make_async_remote_copy(
            src_ref=src, dst_ref=dst, send_sem=send_sem, recv_sem=recv_sem,
            device_id=(my_dp, d), device_id_type=MESH,
        )

    def sent(ref, send_sem):
        remote(ref, ref, send_sem, send_sem, partner).wait_send()

    def came(ref, recv_sem):
        remote(ref, ref, recv_sem, recv_sem, partner).wait_recv()

    def send_raw(p):
        columns = columns_of(p)
        remote(
            grad.at[:, columns], raw.at[kind, :, columns], raw_send, raw_recv.at[kind * hops + p], across
        ).start()

    def send_slots():
        remote(
            slots.at[pl.ds(0, experts)], slots_in.at[kind], slot_send, slot_recv.at[kind], across
        ).start()

    def send_near(p):
        columns = columns_of(p)
        for j in range(1, half):
            i = (my_i + j) % half
            remote(
                send.at[i, :, columns], recv.at[my_i, :, columns], near_send, chunk_recv.at[p], base + i
            ).start()
            remote(
                send_rest.at[i, :, columns], recv_rest.at[my_i, :, columns],
                near_send, chunk_recv.at[p], base + i,
            ).start()

    outside = 2 * (1 - side)
    outside_first = ((outside + c0, outside + 1 - c0), (half - 2 - outside + c0, half - 1 - outside - c0))

    def send_far(p, targets):
        columns, at = columns_of(p), half + c0 * deep + my_k
        for i in targets:
            remote(
                far.at[i, :, columns_of(p, relayed)], recv.at[at, :, columns],
                far_send, chunk_recv.at[p], far_base + i,
            ).start()

    def send_far_rest(targets):
        columns, at = pl.ds(relayed, width - relayed), half + c0 * deep + my_k
        for i in targets:
            remote(
                far_rest.at[i], recv_rest.at[at, :, columns],
                far_send, chunk_recv.at[hops], far_base + i,
            ).start()

    def send_relay(which, p):
        columns = columns_of(p)
        for j in range(1, half):
            i = (my_i + j) % half
            remote(
                relay.at[i, which, :, columns], recv.at[seat_of(which), :, columns],
                relay_send, chunk_recv.at[p], base + i,
            ).start()
            remote(
                relay_rest.at[i, which, :, columns], recv_rest.at[seat_of(which), :, columns],
                relay_send, chunk_recv.at[p], base + i,
            ).start()

    def wait_chunk(p, senders):
        size = edges[p + 1] - edges[p]
        blocks = senders * size // rest * capacity
        if p == hops:
            blocks += 2 * (width - relayed - size)
        elif p > hops:
            blocks -= 2 * size
        came(counter.at[:, 0:blocks], chunk_recv.at[p])

    spread(0, own_row, base)
    spread(1, own_row, far_base)
    near_scales = scales_of(base)
    grad_load.wait()
    load.start()
    pl.semaphore_wait(barrier, 2 + len(close))
    tell(known.at[0], partner)

    @pl.when(inner)
    def _():
        tell(known.at[0], across)
        send_slots()

        for p in range(hops):
            send_raw(p)
        pl.semaphore_wait(known.at[0], 3)
        tell(known.at[1], across)
        tell(known.at[1], behind)

    @pl.when(outer)
    def _():
        tell(known.at[0], behind)
        pl.semaphore_wait(known.at[0], 1)

    for d in close:
        tell(known.at[2], me, d)

    def direct(p):
        columns = columns_of(p)

        def put(i, block):
            send[i, :, columns] = block

        def put_rest(i, block):
            send_rest[i, :, columns] = block

        fill(0, grad[:, columns], near_scales, put, put_rest)
        if p == 0:
            pl.semaphore_wait(known.at[1], 1)
            if close:
                pl.semaphore_wait(known.at[2], len(close))

            @pl.when(outer)
            def _():
                send_slots()
                send_raw(0)

        send_near(p)
        if p > 0:

            @pl.when(outer)
            def _():
                send_raw(p)

    for p in range(chunks):
        direct(p)

    def fill_far(p):
        columns = columns_of(p, relayed)

        def put(i, block):
            far[i, :, columns] = block

        def put_rest(i, block):
            far_rest[i, :, columns] = block

        fill(1, grad[:, columns_of(p)], far_scales, put, put_rest)

    far_scales = scales_of(far_base)

    @pl.when(inner)
    def _():
        for p in range(hops, chunks):
            fill_far(p)
        for targets in outside_first:
            send_far_rest(targets)
            for p in range(hops, chunks):
                send_far(p, targets)

    recv[my_i] = send[my_i]
    recv_rest[my_i] = send_rest[my_i]
    row_peak = jnp.max(jnp.abs(grad[...]).astype(jnp.float32), axis=1, keepdims=True)
    grad_peak = jnp.max(jnp.where(mask_t.T > 0.5, row_peak, 0.0), axis=0, keepdims=True)
    back = 1.0 / pick(scale_in, me)
    own_hidden = pick(scale_hidden, me)

    load.wait()

    def add_product(p, first=False):
        columns, size = columns_of(p), edges[p + 1] - edges[p]
        for s in range(n_exp):
            rest_rows[s * rest:(s + 1) * rest, 0:size] = recv_rest[s, :, columns].astype(jnp.float32)
        block = jnp.concatenate(
            [
                recv[:, :, columns].reshape(n_exp * main, size),
                rest_rows[:, 0:size].astype(jnp.bfloat16),
            ],
            axis=0,
        )
        product = lax.dot_general(
            block, weight[:, columns], (((1,), (1,)), ((), ())), preferred_element_type=jnp.float32
        )
        acc[...] = product if first else acc[...] + product

    def get_ready(which):
        @pl.when(inner)
        def _():
            came(slots_in.at[which], slot_recv.at[which])
            spread(2 + which, lambda e: slots_in[which, pl.ds(e, 1), :], base)

    def pass_on(which, p):
        columns = columns_of(p)

        @pl.when(inner)
        def _():
            came(raw.at[which, :, columns], raw_recv.at[which * hops + p])

            def put(i, block):
                relay[i, which, :, columns] = block

            def put_rest(i, block):
                relay_rest[i, which, :, columns] = block

            fill(2 + which, raw[which, :, columns], near_scales, put, put_rest)
            send_relay(which, p)
            recv[seat_of(which), :, columns] = relay[my_i, which, :, columns]
            recv_rest[seat_of(which), :, columns] = relay_rest[my_i, which, :, columns]

    def multiply(p):
        @pl.when(inner)
        def _():
            wait_chunk(p, half - 1 + deep if p < hops else n_exp - 2)

        @pl.when(outer)
        def _():
            wait_chunk(p, n_exp - 1)

        add_product(p, p == 0)

    for at, (which, p) in enumerate(ORDER):
        if p == 0:
            get_ready(which)
        pass_on(which, p)
        for taken, place in enumerate(TAKE):
            if place == at:
                multiply(taken)
    for p in range(len(TAKE), chunks):
        multiply(p)
    hidden = acc[...] * back
    peak = jnp.max(jnp.max(jnp.abs(hidden), axis=0, keepdims=True), axis=1, keepdims=True)
    lane = lax.broadcasted_iota(jnp.int32, (1, LANES), 1)
    mine[...] = jnp.where(lane < experts, grad_peak, jnp.where(lane == experts + me, peak, 0.0))
    for j in range(everyone - 1):
        peer = jnp.where(j >= turn, j + 1, j)
        pltpu.make_async_remote_copy(
            src_ref=mine, dst_ref=peaks_in.at[here], send_sem=peak_send, recv_sem=peak_recv,
            device_id=(peer % n_dp, peer // n_dp), device_id_type=MESH,
        ).start()
    peaks_in[here] = mine[...]
    scaled = jnp.clip(acc[...] * back * own_hidden, -1.0, 1.0)
    for at in range(n_exp):
        if at < half:
            block, first = side, at * capacity
        else:
            block, first = 1 - side, ((at - half) % deep * 2 + (at - half) // deep) * capacity
        out_ref[block, first:first + main, :] = scaled[at * main:(at + 1) * main].astype(jnp.bfloat16)
        tail = n_exp * main + at * rest
        out_ref[block, first + main:first + capacity, :] = scaled[tail:tail + rest].astype(jnp.bfloat16)

    per_block = capacity // rest
    sent(slots.at[pl.ds(0, experts)], slot_send)
    sent(counter.at[:, 0:(half - 1) * per_block * width], near_send)

    @pl.when(outer)
    def _():
        sent(grad, raw_send)

    @pl.when(inner)
    def _():
        sent(grad.at[:, pl.ds(0, relayed)], raw_send)
        sent(counter.at[:, 0:half * per_block * (width - relayed)], far_send)
        sent(counter.at[:, 0:(half - 1) * per_block * (relayed + width)], relay_send)

    others = peaks_in.at[pl.ds(0, everyone - 1)]
    sent(others, peak_send)
    came(others, peak_recv)
    best_ref[...] = jnp.max(peaks_in[...], axis=0)


def relay_finish(
    hist_g_ref, hist_h_ref, best_ref, out_ref, new_g_hbm, new_h_hbm, final_hbm, new_g, new_h, sem
):
    result = pltpu.make_async_copy(out_ref, final_hbm, sem.at[0])
    result.start()
    keep = hist_g_ref.shape[0] - 1
    experts = hist_g_ref.shape[1]
    new_g[0:keep, :] = hist_g_ref[1:keep + 1, :]
    new_g[keep:keep + 1, :] = best_ref[0:1, 0:experts]
    new_h[0:keep, :] = hist_h_ref[1:keep + 1, :]
    new_h[keep:keep + 1, :] = best_ref[0:1, experts:2 * experts]
    first = pltpu.make_async_copy(new_g, new_g_hbm, sem.at[1])
    second = pltpu.make_async_copy(new_h, new_h_hbm, sem.at[2])
    first.start()
    second.start()
    first.wait()
    second.wait()
    result.wait()


def by_relay(grad_out, expert_ids, down_weight, history_grad, history_hidden):
    tokens, width = grad_out.shape
    experts = history_grad.shape[1]
    n_dp, n_exp = lax.axis_size("dp"), lax.axis_size("expert")
    capacity = tokens * 9 // 32
    main = (capacity - 1) // 16 * 16
    rest = capacity - main
    units = down_weight.shape[1]
    half, deep = n_exp // 2, n_exp // 4
    edges = chunk_edges(width)
    chunks, hops = len(edges) - 1, len(RELAYED)
    span = max(after - before for before, after in zip(edges, edges[1:]))
    tail = width - edges[hops]
    everyone = n_dp * n_exp
    vmem, anywhere = pl.BlockSpec(memory_space=pltpu.VMEM), pl.BlockSpec(memory_space=pl.ANY)
    dma = pltpu.SemaphoreType.DMA
    bf16, f32 = jnp.bfloat16, jnp.float32
    out, best = pl.pallas_call(
        functools.partial(relay_kernel, n_dp, n_exp, experts, capacity),
        out_shape=(pltpu.VMEM((2, half * capacity, units), bf16), pltpu.VMEM((1, LANES), f32)),
        in_specs=[anywhere] * 5,
        out_specs=(vmem, vmem),
        scratch_shapes=[
            pltpu.VMEM((tokens, width), bf16),
            pltpu.VMEM(expert_ids.shape[::-1], jnp.int32),
            pltpu.VMEM(history_grad.shape, f32),
            pltpu.VMEM(history_hidden.shape, f32),
            pltpu.VMEM((deep, tokens, width), bf16),
            pltpu.VMEM((units, width), bf16),
            pltpu.VMEM((half, main, width), bf16),
            pltpu.VMEM((half, rest, width), bf16),
            pltpu.VMEM((half, main, tail), bf16),
            pltpu.VMEM((half, rest, tail), bf16),
            pltpu.VMEM((half, deep, main, width), bf16),
            pltpu.VMEM((half, deep, rest, width), bf16),
            pltpu.VMEM((n_exp, main, width), bf16),
            pltpu.VMEM((n_exp, rest, width), bf16),
            pltpu.VMEM((rest, 2 * half * capacity // rest * width), bf16),
            pltpu.VMEM((n_exp * rest, span), f32),
            pltpu.VMEM((n_exp * capacity, units), f32),
            pltpu.VMEM((LANES, tokens), f32),
            pltpu.VMEM((deep, experts, tokens), f32),
            pltpu.VMEM((2 + deep, half * capacity, tokens), bf16),
            pltpu.VMEM((1, LANES), f32),
            pltpu.VMEM((everyone, 1, LANES), f32),
            dma((5,)), pltpu.SemaphoreType.REGULAR((3,)), dma, dma((deep,)), dma, dma((hops + chunks,)),
            dma, dma, dma,
            dma((chunks,)), dma, dma,
        ],
        compiler_params=pltpu.CompilerParams(
            collective_id=1, has_side_effects=True, vmem_limit_bytes=56 * 1024 * 1024
        ),
    )(grad_out, expert_ids.T, history_grad, history_hidden, down_weight)
    new_g, new_h, out = pl.pallas_call(
        relay_finish,
        out_shape=(
            jax.ShapeDtypeStruct(history_grad.shape, f32),
            jax.ShapeDtypeStruct(history_hidden.shape, f32),
            jax.ShapeDtypeStruct((2, half * capacity, units), bf16),
        ),
        in_specs=[vmem, vmem, vmem, vmem],
        out_specs=(anywhere, anywhere, anywhere),
        scratch_shapes=[
            pltpu.VMEM(history_grad.shape, f32), pltpu.VMEM(history_hidden.shape, f32), dma((3,))
        ],
        compiler_params=pltpu.CompilerParams(vmem_limit_bytes=4 * 1024 * 1024),
    )(history_grad, history_hidden, best, out)
    return out.reshape(1, 1, n_exp * capacity, units), new_g, new_h


def fits_relay(tokens, width, experts, n_exp):
    capacity = tokens * 9 // 32
    return (
        experts == n_exp and n_exp // 4 == 2 and experts % 8 == 0 and 2 * experts <= LANES
        and tokens % LANES == 0 and width % (sum(RELAYED + DIRECT) * LANES) == 0
        and (n_exp // 2 * capacity) % 16 == 0 and (n_exp // 2 * (capacity % 16)) % 16 == 0
        and 0 < capacity % 16 and capacity % (capacity % 16) == 0
    )


def per_device(*arguments):
    (tokens, width), experts = arguments[0].shape, arguments[3].shape[1]
    if fits_relay(tokens, width, experts, lax.axis_size("expert")):
        return by_relay(*arguments)
    return by_blocks(*arguments)


def solution(mesh):
    in_specs = (
        P(("dp", "expert"), None),
        P(("dp", "expert"), None),
        P("expert", None, None),
        P(),
        P(),
    )
    out_specs = (P("dp", "expert", None, None), P(), P())
    return jax.shard_map(
        per_device, mesh=mesh, in_specs=in_specs, out_specs=out_specs, check_vma=False
    )
```

```python
import functools

import jax
import jax.numpy as jnp
from jax import lax
from jax.experimental import pallas as pl
from jax.experimental.pallas import tpu as pltpu
from jax.sharding import PartitionSpec as P

MESH = pl.DeviceIdType.MESH
PARTS = 4
LANES = 128
RELAYED = (3, 3)
DIRECT = (3, 2, 1)
ORDER = ((0, 0), (1, 0), (0, 1), (1, 1), (1, 2), (1, 3), (1, 4))
TAKE = (3,)


def flip_bits(q, k, count):
    out, bit = 0, 1
    while bit < count:
        a, b = (q // bit) % 2, (k // bit) % 2
        out = out + bit * (a + b - 2 * a * b)
        bit *= 2
    return out


def kernel(
    n_dp, n_exp, experts, capacity,
    grad_hbm, ids_ref, hist_g_ref, hist_h_ref, weight_hbm,
    out_ref, best_ref,
    grad_ref, held, weight, send, send_rest, recv, recv_rest, rest_rows, slots, mine, peaks_in,
    grad_sem, weight_sem, send_sem, recv_sem, send_rest_sem, recv_rest_sem, peak_send_sem, peak_recv_sem,
):
    tokens = grad_ref.shape[0]
    main = send.shape[1]
    slices = n_exp // experts
    chips = n_exp // 2
    my_dp, me = lax.axis_index("dp"), lax.axis_index("expert")
    q0, c0 = me // 2, me % 2
    partner = q0 * 2 + 1 - c0
    own = me // slices
    grad_load = pltpu.make_async_copy(grad_hbm, grad_ref, grad_sem)
    grad_load.start()
    load = pltpu.make_async_copy(weight_hbm.at[0], weight, weight_sem)

    barrier = pltpu.get_barrier_semaphore()

    everyone = n_dp * n_exp
    here = my_dp * n_exp + me

    def greet(j, x):
        peer = (here + j) % everyone
        pl.semaphore_signal(
            barrier, inc=1, device_id=(peer // n_exp, peer % n_exp), device_id_type=MESH
        )
        return x

    lax.fori_loop(1, everyone, greet, 0)

    expert_row = lax.broadcasted_iota(jnp.int32, (LANES, tokens), 0)
    ids = ids_ref[...]
    mask_t = jnp.where((ids[0:1, :] == expert_row) | (ids[1:2, :] == expert_row), 1.0, 0.0)
    row = lax.broadcasted_iota(jnp.int32, (tokens, tokens), 0)
    col = lax.broadcasted_iota(jnp.int32, (tokens, tokens), 1)
    earlier = jnp.where(row < col, 1.0, 0.0).astype(jnp.bfloat16)
    before = jnp.dot(mask_t.astype(jnp.bfloat16), earlier, preferred_element_type=jnp.float32)
    slots[...] = jnp.where(mask_t > 0.5, before, -1.0)
    scale_in = 1.0 / jnp.max(hist_g_ref[...], axis=0, keepdims=True)
    scale_hidden = 1.0 / jnp.max(hist_h_ref[...], axis=0, keepdims=True)
    which = lax.broadcasted_iota(jnp.int32, (1, experts), 1)

    def pick(values, e):
        return jnp.sum(jnp.where(which == e, values, 0.0), axis=1, keepdims=True)

    position = lax.broadcasted_iota(jnp.int32, (capacity, tokens), 0).astype(jnp.float32)

    def prepare(e):
        onehot = jnp.where(slots[pl.ds(e, 1), :] == position, 1.0, 0.0).astype(jnp.bfloat16)
        rows = jnp.dot(onehot, grad_ref[...], preferred_element_type=jnp.float32)
        block = jnp.clip(rows * pick(scale_in, e), -1.0, 1.0)
        send[e] = block[0:main].astype(jnp.bfloat16)
        send_rest[e] = block[main:capacity].astype(jnp.bfloat16)

    span = weight.shape[1] // PARTS

    def outgoing(d, p):
        columns = pl.ds(p * span, span)
        return pltpu.make_async_remote_copy(
            src_ref=send.at[d // slices, :, columns], dst_ref=recv.at[me, :, columns],
            send_sem=send_sem.at[p, d], recv_sem=recv_sem.at[p, me],
            device_id=(my_dp, d), device_id_type=MESH,
        )

    def outgoing_rest(d):
        return pltpu.make_async_remote_copy(
            src_ref=send_rest.at[d // slices], dst_ref=recv_rest.at[me],
            send_sem=send_rest_sem.at[d], recv_sem=recv_rest_sem.at[me],
            device_id=(my_dp, d), device_id_type=MESH,
        )

    def incoming(s, p):
        columns = pl.ds(p * span, span)
        return pltpu.make_async_remote_copy(
            src_ref=send.at[0, :, columns], dst_ref=recv.at[s, :, columns],
            send_sem=send_sem.at[p, s], recv_sem=recv_sem.at[p, s],
            device_id=(my_dp, s), device_id_type=MESH,
        )

    def incoming_rest(s):
        return pltpu.make_async_remote_copy(
            src_ref=send_rest.at[0], dst_ref=recv_rest.at[s],
            send_sem=send_rest_sem.at[s], recv_sem=recv_rest_sem.at[s],
            device_id=(my_dp, s), device_id_type=MESH,
        )

    def chip_of(j):
        k = j
        if chips & (chips - 1) == 0:
            return flip_bits(q0, k, chips)
        return (q0 + k) % chips

    def source_of(j):
        if chips & (chips - 1) == 0:
            return chip_of(j)
        k = j
        return (q0 + chips - k) % chips

    def prepare_pair(q):
        prepare(2 * q + c0)
        prepare(2 * q + 1 - c0)

    def send_pair(q):
        for p in range(PARTS):
            for c in (c0, 1 - c0):
                outgoing(2 * q + c, p).start()
                if p == 0:
                    outgoing_rest(2 * q + c).start()

    greeted = everyone - 1
    grad_load.wait()
    load.start()
    if slices == 1:
        prepare_pair(chip_of(jnp.int32(1)))
        pl.semaphore_wait(barrier, greeted)

        def step(j, x):
            prepare_pair(chip_of((j + 1) % chips))
            send_pair(chip_of(j))
            return x
    else:
        def fill(e, x):
            prepare(e)
            return x

        lax.fori_loop(0, experts, fill, 0)
        pl.semaphore_wait(barrier, greeted)

        def step(j, x):
            send_pair(chip_of(j))
            return x

    lax.fori_loop(1, chips, step, 0)
    for p in range(PARTS):
        outgoing(partner, p).start()
    outgoing_rest(partner).start()

    recv[me] = send[own]
    recv_rest[me] = send_rest[own]
    row_peak = jnp.max(jnp.abs(grad_ref[...]).astype(jnp.float32), axis=1, keepdims=True)
    grad_peak = jnp.max(jnp.where(mask_t.T > 0.5, row_peak, 0.0), axis=0, keepdims=True)

    back = 1.0 / pick(scale_in, own)
    own_hidden = pick(scale_hidden, own)
    load.wait()

    def times_weight(block, columns):
        return lax.dot_general(
            block, weight[:, columns], (((1,), (1,)), ((), ())), preferred_element_type=jnp.float32
        )

    def multiply(block):
        return finish(times_weight(block, slice(None)))

    def finish(product):
        hidden = product * back
        scaled = jnp.clip(hidden * own_hidden, -1.0, 1.0)
        return scaled, jnp.max(jnp.max(jnp.abs(hidden), axis=0, keepdims=True), axis=1, keepdims=True)

    def pair_rows(q):
        return recv[pl.ds(2 * q, 2)].reshape(2 * main, recv.shape[2])

    def put_pair(q, scaled):
        for c in range(2):
            held[2 * q + c] = scaled[c * main:(c + 1) * main].astype(jnp.bfloat16)

    def take_own():
        for p in range(PARTS):
            incoming(partner, p).wait_recv()
        scaled, peak = multiply(pair_rows(q0))
        put_pair(q0, scaled)
        return peak

    def take(j, peak):
        q = source_of(j)
        for p in range(PARTS):
            incoming(2 * q, p).wait_recv()
            incoming(2 * q + 1, p).wait_recv()
        scaled, peak_here = multiply(pair_rows(q))
        put_pair(q, scaled)
        return jnp.maximum(peak, peak_here)

    peak = lax.fori_loop(1, chips - 1, take, take_own())

    def take_rest(j, x):
        incoming_rest((me + j) % n_exp).wait_recv()
        return x

    lax.fori_loop(1, n_exp, take_rest, 0)
    rest = capacity - main
    for s in range(n_exp):
        rest_rows[s * rest:(s + 1) * rest, :] = recv_rest[s].astype(jnp.float32)
    last = source_of(jnp.int32(chips - 1))
    product = None
    for p in range(PARTS):
        incoming(2 * last, p).wait_recv()
        incoming(2 * last + 1, p).wait_recv()
        columns = slice(p * span, (p + 1) * span)
        pair = recv[pl.ds(2 * last, 2), :, columns].reshape(2 * main, span)
        block = jnp.concatenate([pair, rest_rows[:, columns].astype(jnp.bfloat16)], axis=0)
        piece = times_weight(block, columns)
        product = piece if product is None else product + piece
    scaled, peak_here = finish(product)
    peak = jnp.maximum(peak, peak_here)

    at = lax.broadcasted_iota(jnp.int32, (1, LANES), 1)
    hidden_peak = jnp.where(at == own, peak, 0.0)
    part = lax.broadcasted_iota(jnp.int32, (8, LANES), 0)
    mine[...] = jnp.where(part == 0, grad_peak, jnp.where(part == 1, hidden_peak, 0.0))

    def peak_copy(peer, slot, j):
        return pltpu.make_async_remote_copy(
            src_ref=mine, dst_ref=peaks_in.at[slot],
            send_sem=peak_send_sem.at[j], recv_sem=peak_recv_sem.at[slot],
            device_id=(peer // n_exp, peer % n_exp), device_id_type=MESH,
        )

    def peak_start(j, x):
        peak_copy((here + j) % everyone, here, j).start()
        return x

    def peak_fold(j, best):
        peer = (here + j) % everyone
        peak_copy(peer, peer, j).wait_recv()
        return jnp.maximum(best, peaks_in[peer])

    def peak_finish(j, x):
        peak_copy((here + j) % everyone, here, j).wait_send()
        return x

    lax.fori_loop(1, everyone, peak_start, 0)
    put_pair(last, scaled)
    for s in range(n_exp):
        at_row = 2 * main + s * rest
        base = s * capacity
        out_ref[base:base + main, :] = held[s]
        out_ref[base + main:base + capacity, :] = scaled[at_row:at_row + rest].astype(jnp.bfloat16)
    best = lax.fori_loop(1, everyone, peak_fold, mine[...])
    lax.fori_loop(1, everyone, peak_finish, 0)

    best_ref[...] = best

    def drain(j, x):
        for p in range(PARTS):
            outgoing((me + j) % n_exp, p).wait_send()
        outgoing_rest((me + j) % n_exp).wait_send()
        return x

    lax.fori_loop(1, n_exp, drain, 0)


def finish_kernel(hist_g_ref, hist_h_ref, best_ref, out_ref, new_g_ref, new_h_ref, final_ref):
    final_ref[...] = out_ref[...]
    keep = hist_g_ref.shape[0] - 1
    experts = hist_g_ref.shape[1]
    new_g_ref[0:keep, :] = hist_g_ref[1:keep + 1, :]
    new_g_ref[keep:keep + 1, :] = best_ref[0:1, 0:experts]
    new_h_ref[0:keep, :] = hist_h_ref[1:keep + 1, :]
    new_h_ref[keep:keep + 1, :] = best_ref[1:2, 0:experts]


def by_blocks(grad_out, expert_ids, down_weight, history_grad, history_hidden):
    tokens, width = grad_out.shape
    experts = history_grad.shape[1]
    n_dp, n_exp = lax.axis_size("dp"), lax.axis_size("expert")
    capacity = tokens * 9 // 32
    main = (capacity - 1) // 16 * 16
    rest = capacity - main
    units = down_weight.shape[1]
    vmem = pl.BlockSpec(memory_space=pltpu.VMEM)
    dma = pltpu.SemaphoreType.DMA
    out, best = pl.pallas_call(
        functools.partial(kernel, n_dp, n_exp, experts, capacity),
        out_shape=(
            jax.ShapeDtypeStruct((n_exp * capacity, units), jnp.bfloat16),
            jax.ShapeDtypeStruct((8, LANES), jnp.float32),
        ),
        in_specs=[pl.BlockSpec(memory_space=pl.ANY), vmem, vmem, vmem, pl.BlockSpec(memory_space=pl.ANY)],
        out_specs=(vmem, vmem),
        scratch_shapes=[
            pltpu.VMEM((tokens, width), jnp.bfloat16),
            pltpu.VMEM((n_exp, main, units), jnp.bfloat16),
            pltpu.VMEM((units, width), jnp.bfloat16),
            pltpu.VMEM((experts, main, width), jnp.bfloat16),
            pltpu.VMEM((experts, rest, width), jnp.bfloat16),
            pltpu.VMEM((n_exp, main, width), jnp.bfloat16),
            pltpu.VMEM((n_exp, rest, width), jnp.bfloat16),
            pltpu.VMEM((n_exp * rest, width), jnp.float32),
            pltpu.VMEM((LANES, tokens), jnp.float32),
            pltpu.VMEM((8, LANES), jnp.float32),
            pltpu.VMEM((n_dp * n_exp, 8, LANES), jnp.float32),
            dma, dma, dma((PARTS, n_exp)), dma((PARTS, n_exp)), dma((n_exp,)), dma((n_exp,)),
            dma((n_dp * n_exp,)), dma((n_dp * n_exp,)),
        ],
        compiler_params=pltpu.CompilerParams(
            collective_id=0, has_side_effects=True, vmem_limit_bytes=60 * 1024 * 1024
        ),
    )(grad_out, expert_ids.T, history_grad, history_hidden, down_weight)
    new_g, new_h, out = pl.pallas_call(
        finish_kernel,
        out_shape=(
            jax.ShapeDtypeStruct(history_grad.shape, jnp.float32),
            jax.ShapeDtypeStruct(history_hidden.shape, jnp.float32),
            jax.ShapeDtypeStruct(out.shape, out.dtype),
        ),
        in_specs=[vmem, vmem, vmem, vmem],
        out_specs=(vmem, vmem, vmem),
    )(history_grad, history_hidden, best, out)
    return out.reshape(1, 1, n_exp * capacity, units), new_g, new_h


def chunk_edges(width):
    unit, edges = width // sum(RELAYED + DIRECT), [0]
    for pieces in RELAYED + DIRECT:
        edges.append(edges[-1] + pieces * unit)
    return edges


def relay_kernel(
    n_dp, n_exp, experts, capacity,
    grad_hbm, ids_hbm, hist_g_hbm, hist_h_hbm, weight_hbm,
    out_ref, best_ref,
    grad, ids_ref, hist_g_ref, hist_h_ref, raw, weight,
    send, send_rest, far, far_rest, relay, relay_rest, recv, recv_rest,
    counter, rest_rows, acc, slots, slots_in, onehot, mine, peaks_in,
    load_sem, known, slot_send, slot_recv, raw_send, raw_recv,
    near_send, far_send, relay_send,
    chunk_recv, peak_send, peak_recv,
):
    tokens, width = grad.shape
    main = send.shape[1]
    rest = capacity - main
    half, deep = n_exp // 2, n_exp // 4
    edges = chunk_edges(width)
    hops, chunks = len(RELAYED), len(edges) - 1
    relayed = edges[hops]
    my_dp, me = lax.axis_index("dp"), lax.axis_index("expert")
    q0, c0 = me // 2, me % 2
    side = q0 // deep
    base, far_base = side * half, (1 - side) * half
    my_i, my_k = me - base, q0 - side * deep
    inner = q0 == deep - 1 + side
    outer = jnp.logical_not(inner)
    partner = q0 * 2 + 1 - c0
    kind = jnp.where(inner, 0, 1)

    def seat_of(which):
        return half + c0 * deep + side + which - 2 * side * which

    across = 2 * (deep - side) + c0
    behind = 2 * (deep - 1 + side + jnp.where(inner, 2 * side - 1, 0)) + c0
    everyone = n_dp * n_exp
    here = my_dp * n_exp + me
    turn = me * n_dp + my_dp

    def loading(src, dst, at):
        return pltpu.make_async_copy(src, dst, load_sem.at[at])

    small = (
        loading(ids_hbm, ids_ref, 0), loading(hist_g_hbm, hist_g_ref, 1), loading(hist_h_hbm, hist_h_ref, 2)
    )
    grad_load = loading(grad_hbm, grad, 3)
    load = loading(weight_hbm.at[0], weight, 4)
    for copy in small:
        copy.start()
    grad_load.start()

    def tell(semaphore, d, dp=None):
        pl.semaphore_signal(
            semaphore, inc=1, device_id=(my_dp if dp is None else dp, d), device_id_type=MESH
        )

    barrier = pltpu.get_barrier_semaphore()

    @pl.when(inner)
    def _():
        tell(barrier, across)
        tell(barrier, behind)

    tell(barrier, partner)
    if n_dp in (2, 4):
        close = [flip_bits(my_dp, bit, n_dp) for bit in (1, 2) if bit < n_dp]
    else:
        close = [(my_dp + d) % n_dp for d in range(1, n_dp)]
    for d in close:
        tell(barrier, me, d)

    expert_row = lax.broadcasted_iota(jnp.int32, (LANES, tokens), 0)
    row = lax.broadcasted_iota(jnp.int32, (tokens, tokens), 0)
    col = lax.broadcasted_iota(jnp.int32, (tokens, tokens), 1)
    earlier = jnp.where(row < col, 1.0, 0.0).astype(jnp.bfloat16)
    for copy in small:
        copy.wait()
    ids = ids_ref[...]
    mask_t = jnp.where((ids[0:1, :] == expert_row) | (ids[1:2, :] == expert_row), 1.0, 0.0)
    before = jnp.dot(mask_t.astype(jnp.bfloat16), earlier, preferred_element_type=jnp.float32)
    slots[...] = jnp.where(mask_t > 0.5, before, -1.0)
    scale_in = 1.0 / jnp.max(hist_g_ref[...], axis=0, keepdims=True)
    scale_hidden = 1.0 / jnp.max(hist_h_ref[...], axis=0, keepdims=True)
    which = lax.broadcasted_iota(jnp.int32, (1, experts), 1)

    def pick(values, e):
        return jnp.sum(jnp.where(which == e, values, 0.0), axis=1, keepdims=True)

    position = lax.broadcasted_iota(jnp.int32, (main, tokens), 0).astype(jnp.float32)
    rest_row = lax.broadcasted_iota(jnp.int32, (half * rest, tokens), 0)
    rest_position = (rest_row % rest + main).astype(jnp.float32)
    rest_group = rest_row // rest

    def spread(at, slot_row, first):
        spare = jnp.full((half * rest, tokens), -1.0, jnp.float32)
        for i in range(half):
            named = slot_row(first + i)
            onehot[at, i * main:(i + 1) * main, :] = jnp.where(
                named == position, 1.0, 0.0
            ).astype(jnp.bfloat16)
            spare = jnp.where(rest_group == i, named, spare)
        onehot[at, half * main:half * capacity, :] = jnp.where(
            spare == rest_position, 1.0, 0.0
        ).astype(jnp.bfloat16)

    def own_row(e):
        return slots[pl.ds(e, 1), :]

    group_column = lax.broadcasted_iota(jnp.int32, (half * rest, 1), 0) // rest

    def scales_of(first):
        scales = [pick(scale_in, first + i) for i in range(half)]
        spare = jnp.zeros((half * rest, 1), jnp.float32)
        for i in range(half):
            spare = jnp.where(group_column == i, scales[i], spare)
        return scales, spare

    def fill(at, source, scales, put, put_rest):
        rows = jnp.dot(onehot[at], source, preferred_element_type=jnp.float32)
        each, spare = scales
        for i in range(half):
            put(i, jnp.clip(rows[i * main:(i + 1) * main] * each[i], -1.0, 1.0).astype(jnp.bfloat16))
        ends = jnp.clip(rows[half * main:half * capacity] * spare, -1.0, 1.0)
        for i in range(half):
            put_rest(i, ends[i * rest:(i + 1) * rest].astype(jnp.bfloat16))

    def columns_of(p, origin=0):
        return slice(edges[p] - origin, edges[p + 1] - origin)

    def remote(src, dst, send_sem, recv_sem, d):
        return pltpu.make_async_remote_copy(
            src_ref=src, dst_ref=dst, send_sem=send_sem, recv_sem=recv_sem,
            device_id=(my_dp, d), device_id_type=MESH,
        )

    def sent(ref, send_sem):
        remote(ref, ref, send_sem, send_sem, partner).wait_send()

    def came(ref, recv_sem):
        remote(ref, ref, recv_sem, recv_sem, partner).wait_recv()

    def send_raw(p):
        columns = columns_of(p)
        remote(
            grad.at[:, columns], raw.at[kind, :, columns], raw_send, raw_recv.at[kind * hops + p], across
        ).start()

    def send_slots():
        remote(
            slots.at[pl.ds(0, experts)], slots_in.at[kind], slot_send, slot_recv.at[kind], across
        ).start()

    def send_near(p):
        columns = columns_of(p)
        for j in range(1, half):
            i = (my_i + j) % half
            remote(
                send.at[i, :, columns], recv.at[my_i, :, columns], near_send, chunk_recv.at[p], base + i
            ).start()
            remote(
                send_rest.at[i, :, columns], recv_rest.at[my_i, :, columns],
                near_send, chunk_recv.at[p], base + i,
            ).start()

    outside = 2 * (1 - side)
    outside_first = ((outside + c0, outside + 1 - c0), (half - 2 - outside + c0, half - 1 - outside - c0))

    def send_far(first, after, targets):
        at = half + c0 * deep + my_k
        for i in targets:
            remote(
                far.at[i, :, pl.ds(edges[first] - relayed, edges[after] - edges[first])],
                recv.at[at, :, pl.ds(edges[first], edges[after] - edges[first])],
                far_send, chunk_recv.at[first], far_base + i,
            ).start()

    def send_far_rest(targets):
        columns, at = pl.ds(relayed, width - relayed), half + c0 * deep + my_k
        for i in targets:
            remote(
                far_rest.at[i], recv_rest.at[at, :, columns],
                far_send, chunk_recv.at[hops], far_base + i,
            ).start()

    def send_relay(which, p):
        columns = columns_of(p)
        for j in range(1, half):
            i = (my_i + j) % half
            remote(
                relay.at[i, which, :, columns], recv.at[seat_of(which), :, columns],
                relay_send, chunk_recv.at[p], base + i,
            ).start()
            remote(
                relay_rest.at[i, which, :, columns], recv_rest.at[seat_of(which), :, columns],
                relay_send, chunk_recv.at[p], base + i,
            ).start()

    def wait_chunk(p, senders, ahead):
        size = edges[p + 1] - edges[p]
        blocks = senders * size // rest * capacity
        if p == hops:
            blocks += 2 * (width - relayed - size) // rest * ahead
        elif p > hops:
            blocks -= 2 * size // rest * ahead
        came(counter.at[:, 0:blocks], chunk_recv.at[p])

    spread(0, own_row, base)
    spread(1, own_row, far_base)
    near_scales = scales_of(base)
    grad_load.wait()
    load.start()
    pl.semaphore_wait(barrier, 2 + len(close))
    tell(known.at[0], partner)

    @pl.when(inner)
    def _():
        tell(known.at[0], across)
        send_slots()

        for p in range(hops):
            send_raw(p)
        pl.semaphore_wait(known.at[0], 3)
        tell(known.at[1], across)
        tell(known.at[1], behind)

    @pl.when(outer)
    def _():
        tell(known.at[0], behind)
        pl.semaphore_wait(known.at[0], 1)

    for d in close:
        tell(known.at[2], me, d)

    def direct(p):
        columns = columns_of(p)

        def put(i, block):
            send[i, :, columns] = block

        def put_rest(i, block):
            send_rest[i, :, columns] = block

        fill(0, grad[:, columns], near_scales, put, put_rest)
        if p == 0:
            pl.semaphore_wait(known.at[1], 1)
            if close:
                pl.semaphore_wait(known.at[2], len(close))

            @pl.when(outer)
            def _():
                send_slots()
                send_raw(0)

        send_near(p)
        if p > 0:

            @pl.when(outer)
            def _():
                send_raw(p)

    for p in range(chunks):
        direct(p)

    def fill_far(p):
        columns = columns_of(p, relayed)

        def put(i, block):
            far[i, :, columns] = block

        def put_rest(i, block):
            far_rest[i, :, columns] = block

        fill(1, grad[:, columns_of(p)], far_scales, put, put_rest)

    far_scales = scales_of(far_base)

    @pl.when(inner)
    def _():
        for p in range(hops, chunks):
            fill_far(p)
        for targets in outside_first:
            send_far_rest(targets)
        send_far(hops, chunks, outside_first[0])
        for p in range(hops, chunks):
            send_far(p, p + 1, outside_first[1])

    recv[my_i] = send[my_i]
    recv_rest[my_i] = send_rest[my_i]
    row_peak = jnp.max(jnp.abs(grad[...]).astype(jnp.float32), axis=1, keepdims=True)
    grad_peak = jnp.max(jnp.where(mask_t.T > 0.5, row_peak, 0.0), axis=0, keepdims=True)
    back = 1.0 / pick(scale_in, me)
    own_hidden = pick(scale_hidden, me)

    load.wait()

    def add_product(p, first=False):
        columns, size = columns_of(p), edges[p + 1] - edges[p]
        for s in range(n_exp):
            rest_rows[s * rest:(s + 1) * rest, 0:size] = recv_rest[s, :, columns].astype(jnp.float32)
        block = jnp.concatenate(
            [
                recv[:, :, columns].reshape(n_exp * main, size),
                rest_rows[:, 0:size].astype(jnp.bfloat16),
            ],
            axis=0,
        )
        product = lax.dot_general(
            block, weight[:, columns], (((1,), (1,)), ((), ())), preferred_element_type=jnp.float32
        )
        acc[...] = product if first else acc[...] + product

    def get_ready(which):
        @pl.when(inner)
        def _():
            came(slots_in.at[which], slot_recv.at[which])
            spread(2 + which, lambda e: slots_in[which, pl.ds(e, 1), :], base)

    def pass_on(which, p):
        columns = columns_of(p)

        @pl.when(inner)
        def _():
            came(raw.at[which, :, columns], raw_recv.at[which * hops + p])

            def put(i, block):
                relay[i, which, :, columns] = block

            def put_rest(i, block):
                relay_rest[i, which, :, columns] = block

            fill(2 + which, raw[which, :, columns], near_scales, put, put_rest)
            send_relay(which, p)
            recv[seat_of(which), :, columns] = relay[my_i, which, :, columns]
            recv_rest[seat_of(which), :, columns] = relay_rest[my_i, which, :, columns]

    def multiply(p):
        @pl.when(inner)
        def _():
            wait_chunk(p, half - 1 + deep if p < hops else n_exp - 2, rest)

        @pl.when(outer)
        def _():
            wait_chunk(p, n_exp - 1, capacity)

        add_product(p, p == 0)

    for at, (which, p) in enumerate(ORDER):
        if p == 0:
            get_ready(which)
        pass_on(which, p)
        for taken, place in enumerate(TAKE):
            if place == at:
                multiply(taken)
    for p in range(len(TAKE), chunks):
        multiply(p)
    hidden = acc[...] * back
    peak = jnp.max(jnp.max(jnp.abs(hidden), axis=0, keepdims=True), axis=1, keepdims=True)
    lane = lax.broadcasted_iota(jnp.int32, (1, LANES), 1)
    mine[...] = jnp.where(lane < experts, grad_peak, jnp.where(lane == experts + me, peak, 0.0))
    for j in range(everyone - 1):
        peer = jnp.where(j >= turn, j + 1, j)
        pltpu.make_async_remote_copy(
            src_ref=mine, dst_ref=peaks_in.at[here], send_sem=peak_send, recv_sem=peak_recv,
            device_id=(peer % n_dp, peer // n_dp), device_id_type=MESH,
        ).start()
    peaks_in[here] = mine[...]
    scaled = jnp.clip(acc[...] * back * own_hidden, -1.0, 1.0)
    for at in range(n_exp):
        if at < half:
            block, first = side, at * capacity
        else:
            block, first = 1 - side, ((at - half) % deep * 2 + (at - half) // deep) * capacity
        out_ref[block, first:first + main, :] = scaled[at * main:(at + 1) * main].astype(jnp.bfloat16)
        tail = n_exp * main + at * rest
        out_ref[block, first + main:first + capacity, :] = scaled[tail:tail + rest].astype(jnp.bfloat16)

    per_block = capacity // rest
    sent(slots.at[pl.ds(0, experts)], slot_send)
    sent(counter.at[:, 0:(half - 1) * per_block * width], near_send)

    @pl.when(outer)
    def _():
        sent(grad, raw_send)

    @pl.when(inner)
    def _():
        sent(grad.at[:, pl.ds(0, relayed)], raw_send)
        sent(counter.at[:, 0:half * per_block * (width - relayed)], far_send)
        sent(counter.at[:, 0:(half - 1) * per_block * (relayed + width)], relay_send)

    others = peaks_in.at[pl.ds(0, everyone - 1)]
    sent(others, peak_send)
    came(others, peak_recv)
    best_ref[...] = jnp.max(peaks_in[...], axis=0)


def relay_finish(
    hist_g_ref, hist_h_ref, best_ref, out_ref, new_g_hbm, new_h_hbm, final_hbm, new_g, new_h, sem
):
    result = pltpu.make_async_copy(out_ref, final_hbm, sem.at[0])
    result.start()
    keep = hist_g_ref.shape[0] - 1
    experts = hist_g_ref.shape[1]
    new_g[0:keep, :] = hist_g_ref[1:keep + 1, :]
    new_g[keep:keep + 1, :] = best_ref[0:1, 0:experts]
    new_h[0:keep, :] = hist_h_ref[1:keep + 1, :]
    new_h[keep:keep + 1, :] = best_ref[0:1, experts:2 * experts]
    first = pltpu.make_async_copy(new_g, new_g_hbm, sem.at[1])
    second = pltpu.make_async_copy(new_h, new_h_hbm, sem.at[2])
    first.start()
    second.start()
    first.wait()
    second.wait()
    result.wait()


def by_relay(grad_out, expert_ids, down_weight, history_grad, history_hidden):
    tokens, width = grad_out.shape
    experts = history_grad.shape[1]
    n_dp, n_exp = lax.axis_size("dp"), lax.axis_size("expert")
    capacity = tokens * 9 // 32
    main = (capacity - 1) // 16 * 16
    rest = capacity - main
    units = down_weight.shape[1]
    half, deep = n_exp // 2, n_exp // 4
    edges = chunk_edges(width)
    chunks, hops = len(edges) - 1, len(RELAYED)
    span = max(after - before for before, after in zip(edges, edges[1:]))
    tail = width - edges[hops]
    everyone = n_dp * n_exp
    vmem, anywhere = pl.BlockSpec(memory_space=pltpu.VMEM), pl.BlockSpec(memory_space=pl.ANY)
    dma = pltpu.SemaphoreType.DMA
    bf16, f32 = jnp.bfloat16, jnp.float32
    out, best = pl.pallas_call(
        functools.partial(relay_kernel, n_dp, n_exp, experts, capacity),
        out_shape=(pltpu.VMEM((2, half * capacity, units), bf16), pltpu.VMEM((1, LANES), f32)),
        in_specs=[anywhere] * 5,
        out_specs=(vmem, vmem),
        scratch_shapes=[
            pltpu.VMEM((tokens, width), bf16),
            pltpu.VMEM(expert_ids.shape[::-1], jnp.int32),
            pltpu.VMEM(history_grad.shape, f32),
            pltpu.VMEM(history_hidden.shape, f32),
            pltpu.VMEM((deep, tokens, width), bf16),
            pltpu.VMEM((units, width), bf16),
            pltpu.VMEM((half, main, width), bf16),
            pltpu.VMEM((half, rest, width), bf16),
            pltpu.VMEM((half, main, tail), bf16),
            pltpu.VMEM((half, rest, tail), bf16),
            pltpu.VMEM((half, deep, main, width), bf16),
            pltpu.VMEM((half, deep, rest, width), bf16),
            pltpu.VMEM((n_exp, main, width), bf16),
            pltpu.VMEM((n_exp, rest, width), bf16),
            pltpu.VMEM((rest, 2 * half * capacity // rest * width), bf16),
            pltpu.VMEM((n_exp * rest, span), f32),
            pltpu.VMEM((n_exp * capacity, units), f32),
            pltpu.VMEM((LANES, tokens), f32),
            pltpu.VMEM((deep, experts, tokens), f32),
            pltpu.VMEM((2 + deep, half * capacity, tokens), bf16),
            pltpu.VMEM((1, LANES), f32),
            pltpu.VMEM((everyone, 1, LANES), f32),
            dma((5,)), pltpu.SemaphoreType.REGULAR((3,)), dma, dma((deep,)), dma, dma((hops + chunks,)),
            dma, dma, dma,
            dma((chunks,)), dma, dma,
        ],
        compiler_params=pltpu.CompilerParams(
            collective_id=1, has_side_effects=True, vmem_limit_bytes=56 * 1024 * 1024
        ),
    )(grad_out, expert_ids.T, history_grad, history_hidden, down_weight)
    new_g, new_h, out = pl.pallas_call(
        relay_finish,
        out_shape=(
            jax.ShapeDtypeStruct(history_grad.shape, f32),
            jax.ShapeDtypeStruct(history_hidden.shape, f32),
            jax.ShapeDtypeStruct((2, half * capacity, units), bf16),
        ),
        in_specs=[vmem, vmem, vmem, vmem],
        out_specs=(anywhere, anywhere, anywhere),
        scratch_shapes=[
            pltpu.VMEM(history_grad.shape, f32), pltpu.VMEM(history_hidden.shape, f32), dma((3,))
        ],
        compiler_params=pltpu.CompilerParams(vmem_limit_bytes=4 * 1024 * 1024),
    )(history_grad, history_hidden, best, out)
    return out.reshape(1, 1, n_exp * capacity, units), new_g, new_h


def fits_relay(tokens, width, experts, n_exp):
    capacity = tokens * 9 // 32
    return (
        experts == n_exp and n_exp // 4 == 2 and experts % 8 == 0 and 2 * experts <= LANES
        and tokens % LANES == 0 and width % (sum(RELAYED + DIRECT) * LANES) == 0
        and (n_exp // 2 * capacity) % 16 == 0 and (n_exp // 2 * (capacity % 16)) % 16 == 0
        and 0 < capacity % 16 and capacity % (capacity % 16) == 0
    )


def per_device(*arguments):
    (tokens, width), experts = arguments[0].shape, arguments[3].shape[1]
    if fits_relay(tokens, width, experts, lax.axis_size("expert")):
        return by_relay(*arguments)
    return by_blocks(*arguments)


def solution(mesh):
    in_specs = (
        P(("dp", "expert"), None),
        P(("dp", "expert"), None),
        P("expert", None, None),
        P(),
        P(),
    )
    out_specs = (P("dp", "expert", None, None), P(), P())
    return jax.shard_map(
        per_device, mesh=mesh, in_specs=in_specs, out_specs=out_specs, check_vma=False
    )
```
